16 devices in a mesh: rep: 2 (over y, z), dp: 8 (over x, core).
Axes of the slice: x: 4, y: 2, z: 1, core: 2. Of those that a mesh axis runs over, the one named last changes fastest.
The devices are a block of a 4x4x8 slice.
Arguments:
- x: bfloat16 [16, 2048, 1024], P(('rep', 'dp')), parts along dimension 0
- dy: bfloat16 [16, 2048, 1024], P(('rep', 'dp')), parts along dimension 0
- w_gate: bfloat16 [2, 1024, 2816], P(None, 'dp')
- w_up: bfloat16 [2, 1024, 2816], P(None, 'dp')
- w_down: bfloat16 [2, 2816, 1024], P(None, 'dp')
- m_w_gate: float32 [2, 1024, 2816], P(None, 'dp')
- m_w_up: float32 [2, 1024, 2816], P(None, 'dp')
- m_w_down: float32 [2, 2816, 1024], P(None, 'dp')
- v_w_gate: float32 [2, 1024, 2816], P(None, 'dp')
- v_w_up: float32 [2, 1024, 2816], P(None, 'dp')
- v_w_down: float32 [2, 2816, 1024], P(None, 'dp')
Outputs:
- output 1: bfloat16 [4, 1024, 2816], P('rep', 'dp'), parts along dimension 0
- output 2: bfloat16 [4, 1024, 2816], P('rep', 'dp'), parts along dimension 0
- output 3: bfloat16 [4, 2816, 1024], P('rep', 'dp'), parts along dimension 0
- output 4: float32 [4, 1024, 2816], P('rep', 'dp'), parts along dimension 0
- output 5: float32 [4, 1024, 2816], P('rep', 'dp'), parts along dimension 0
- output 6: float32 [4, 2816, 1024], P('rep', 'dp'), parts along dimension 0
- output 7: float32 [4, 1024, 2816], P('rep', 'dp'), parts along dimension 0
- output 8: float32 [4, 1024, 2816], P('rep', 'dp'), parts along dimension 0
- output 9: float32 [4, 2816, 1024], P('rep', 'dp'), parts along dimension 0
There are 2 independent parts. The reference program is written for one: setup_inputs(seed, part) draws one part's arguments, and reference() takes and returns one part's arrays. A program takes and returns all parts, laid end to end along the dimension named above; an argument that names none is the same for every part.
All inputs are finite; a program needn't handle non-finite values.
Results may differ from the reference program's by a relative error of at most 0.022.
Values are sent between devices in bfloat16 or wider.
A program may use at most 768 MiB of HBM per device.

```python
import jax
import jax.numpy as jnp
from jax import lax

SEQUENCES = 8
TOKENS = 2048
D = 1024
FF = 2816
LAYERS = 2
NAMES = ("w_gate", "w_up", "w_down")
SHAPES = {"w_gate": (LAYERS, D, FF), "w_up": (LAYERS, D, FF), "w_down": (LAYERS, FF, D)}


def bump(key, n, height):
    away = (jnp.arange(n, dtype=jnp.int32) - jax.random.randint(key, (), 0, n, jnp.int32)) % n
    return jnp.where(away < n // 8, height, 1.0)


def together(key, own, strength):
    shared = jax.random.normal(key, own.shape[1:], jnp.float32)
    return (own + strength * shared) * lax.rsqrt(1 + strength * strength)


def setup_inputs(seed: int = 0, part: int = 0) -> dict:
    kx, kdy, ka, kb, kz, kf, kh, kl, *keys = jax.random.split(jax.random.key(seed), 8 + 3 * len(NAMES))
    kx, kdy, ka, kb = (jax.random.fold_in(k, part) for k in (kx, kdy, ka, kb))
    kw, km, kv = (keys[i::3] for i in range(3))
    shape = (SEQUENCES, TOKENS, D)
    much_x, much_dy = jax.random.uniform(kz, (2,), jnp.float32, 0.0, 1.0)
    loud = 2.0 ** jax.random.uniform(jax.random.fold_in(kz, 1), (), jnp.float32, -1.0, 2.0)
    layers = 2.0 ** jax.random.uniform(kl, (LAYERS, 1, 1), jnp.float32, -1.0, 1.0)
    x = together(ka, jax.random.normal(kx, shape, jnp.float32), much_x) * bump(kf, D, 4.0)
    dy = together(kb, jax.random.normal(kdy, shape, jnp.float32), much_dy)
    drawn = {"x": x.astype(jnp.bfloat16), "dy": (loud * dy * (SEQUENCES * TOKENS) ** -0.5).astype(jnp.bfloat16)}
    for key, name in zip(kw, NAMES, strict=True):
        w = jax.random.normal(key, SHAPES[name], jnp.float32) * SHAPES[name][1] ** -0.5
        drawn[name] = (w * {"w_gate": 1.0, "w_up": bump(kh, FF, 4.0), "w_down": layers}[name]).astype(jnp.bfloat16)
    for key, name in zip(km, NAMES, strict=True):
        drawn[f"m_{name}"] = 0.1 * jax.random.normal(key, SHAPES[name], jnp.float32)
    for key, name in zip(kv, NAMES, strict=True):
        drawn[f"v_{name}"] = jax.random.uniform(key, SHAPES[name], jnp.float32, 0.005, 0.015)
    return drawn


def matmul(a, w):
    return jnp.dot(a, w, preferred_element_type=jnp.float32).astype(jnp.bfloat16)


def normed(h):
    wide = h.astype(jnp.float32)
    scale = lax.rsqrt(jnp.mean(wide**2, -1, keepdims=True) + 1e-6)
    return (wide * scale).astype(jnp.bfloat16)


def layer(h, w):
    a = normed(h)
    gate = jnp.dot(a, w["w_gate"], preferred_element_type=jnp.float32)
    up = jnp.dot(a, w["w_up"], preferred_element_type=jnp.float32)
    return h + matmul((jax.nn.silu(gate) * up).astype(jnp.bfloat16), w["w_down"])


def adamw(w, m, v, g):
    m = 0.9 * m + 0.1 * g
    v = 0.95 * v + 0.05 * g * g
    step = m * lax.rsqrt(v + 1e-8) + 0.1 * w
    return (w - 0.02 * step).astype(jnp.bfloat16), m, v


def clipped(gradients, sum_of_squares, count):
    factor = jnp.minimum(1.0, 0.5 * lax.rsqrt(sum_of_squares / count + 1e-30))
    return [g * factor for g in gradients]


def stack(weights, h):
    return lax.scan(lambda h, w: (layer(h, w), None), h, weights)[0]


def reference(x, dy, w_gate, w_up, w_down, m_w_gate, m_w_up, m_w_down, v_w_gate, v_w_up, v_w_down):
    weights = dict(zip(NAMES, (w_gate, w_up, w_down), strict=True))

    def take(so_far, sequence):
        h, by_y = sequence
        _, back = jax.vjp(lambda w: stack(w, h), weights)
        return jax.tree.map(lambda total, term: total + term.astype(jnp.float32), so_far, back(by_y)[0]), None

    none_yet = {name: jnp.zeros(w.shape, jnp.float32) for name, w in weights.items()}
    by_weights, _ = lax.scan(take, none_yet, (x, dy))
    gradients = [by_weights[name].astype(jnp.bfloat16).astype(jnp.float32) for name in NAMES]
    gradients = clipped(gradients, sum(jnp.sum(g * g) for g in gradients), sum(g.size for g in gradients))
    new = [
        adamw(w.astype(jnp.float32), m, v, g)
        for w, m, v, g in zip((w_gate, w_up, w_down), (m_w_gate, m_w_up, m_w_down), (v_w_gate, v_w_up, v_w_down), gradients, strict=True)
    ]
    return tuple(one[which] for which in range(3) for one in new)
```

```python
import functools

import jax
import jax.numpy as jnp
from jax import lax
from jax.experimental import pallas as pl
from jax.experimental.pallas import tpu as pltpu
from jax.sharding import PartitionSpec as P

MESH = pl.DeviceIdType.MESH
F32, BF16 = jnp.float32, jnp.bfloat16
ROWS = 32
BLOCK = 512
OWN, DEEP = 4, 3


def dot(a, b):
    return lax.dot_general(a, b, (((1,), (0,)), ((), ())), preferred_element_type=F32)


def dot_t(a, b):
    return lax.dot_general(a, b, (((1,), (1,)), ((), ())), preferred_element_type=F32)


def kernel(
    n, count,
    x, dy, wg, wu, wd,
    gath, act_st, sgu_st, a0t_st, gg, gu, gd, fac,
    va, vat, vc, vct, acc, act, sgu, dgu, wgu_b, wd_b,
    own, term, pair, part, fin, halves, wholes, squares, norms,
    in_sem, own_send, own_local, full_recv, half_recv, part_recv, fwd_send, load_sem, stash_sem, saved_sem,
    pair_send, pair_recv, b_send, b_recv, c_send, c_recv, norm_send, norm_recv,
    pair_free, b_free, c_free,
):
    me = lax.axis_index("dp")
    chips = n // 2
    c, at = lax.rem(me, 2), lax.div(me, 2)
    over = lax.rem(at + 2, chips)
    right_chip, left_chip = lax.rem(at + 1, chips), lax.rem(at + chips - 1, chips)
    partner = at * 2 + 1 - c
    right, left, far = right_chip * 2 + c, left_chip * 2 + c, over * 2 + c
    tokens, d = va.shape
    wide = wgu_b.shape[3] // 2
    slots = wd.shape[1] // ROWS
    layers = wd.shape[0]
    chunks = layers * slots
    blocks = tokens // BLOCK
    high = own.shape[1]
    mid = high // 2
    tall = wg.shape[1]

    def remote(src, dst, send, recv, to):
        return pltpu.make_async_remote_copy(
            src_ref=src, dst_ref=dst, send_sem=send, recv_sem=recv, device_id={"dp": to}, device_id_type=MESH
        )

    def prepare(k):
        b, layer, s = lax.rem(k, OWN), lax.div(k, slots), lax.rem(k, slots)
        lanes = lax.broadcasted_iota(jnp.int32, (tall, 128), 1) // ROWS
        for w, base in ((wg, 0), (wu, wide)):
            for group in range(n // 4):
                total = None
                for place in range(4):
                    unit = slots * (4 * group + place) + s
                    piece = w[layer, :, pl.ds(pl.multiple_of(lax.div(unit, 4) * 128, 128), 128)].astype(F32)
                    piece = pltpu.roll(piece, lax.rem(place + 4 - lax.rem(unit, 4), 4) * ROWS, 1)
                    total = piece if total is None else jnp.where(lanes == place, piece, total)
                own[b, 0:tall, base + 128 * group : base + 128 * (group + 1)] = total.astype(BF16)
        rows = wd[layer, pl.ds(pl.multiple_of(s * ROWS, ROWS), ROWS), :]
        own[b, tall : tall + ROWS, :] = rows[:, : 2 * wide]
        own[b, tall + ROWS : high, :] = rows[:, 2 * wide :]

    def own_copies(k):
        b = lax.rem(k, OWN)
        return [
            remote(own.at[b], gath.at[k, me], own_send.at[b, 0], full_recv.at[b, 0], right),
            remote(own.at[b], gath.at[k, me], own_send.at[b, 1], full_recv.at[b, 1], left),
            remote(own.at[b], gath.at[k, me], own_send.at[b, 2], part_recv.at[b, 0], partner),
        ]

    def own_here(k):
        b = lax.rem(k, OWN)
        return pltpu.make_async_copy(own.at[b], gath.at[k, me], own_local.at[b])

    def e1(k):
        for copy in own_copies(k):
            copy.start()
        own_here(k).start()

        @pl.when(k + 1 < chunks)
        def _():
            @pl.when(k + 1 >= OWN)
            def _():
                for copy in own_copies(k + 1 - OWN):
                    copy.wait_send()

            prepare(k + 1)

    def arrived(region, recv):
        remote(region, region, fwd_send.at[0, 0], recv, me).wait_recv()

    def forwards(k):
        b = lax.rem(k, OWN)
        return [
            remote(gath.at[k, left, 0:mid], gath.at[k, left, 0:mid], fwd_send.at[b, 0], half_recv.at[b, 0], right),
            remote(gath.at[k, right, mid:high], gath.at[k, right, mid:high], fwd_send.at[b, 1], half_recv.at[b, 1], left),
            remote(gath.at[k, left], gath.at[k, left], fwd_send.at[b, 2], part_recv.at[b, 1], partner),
            remote(gath.at[k, right], gath.at[k, right], fwd_send.at[b, 3], part_recv.at[b, 2], partner),
        ]

    def last_forward(k):
        b = lax.rem(k, OWN)
        return remote(gath.at[k, far], gath.at[k, far], fwd_send.at[b, 4], part_recv.at[b, 3], partner)

    def e2(k):
        b = lax.rem(k, OWN)

        @pl.when(k >= OWN)
        def _():
            for copy in forwards(k - OWN):
                copy.wait_send()

        arrived(gath.at[k, left], full_recv.at[b, 0])
        arrived(gath.at[k, right], full_recv.at[b, 1])
        for copy in forwards(k):
            copy.start()

    def e3(k):
        b = lax.rem(k, OWN)

        @pl.when(k >= OWN)
        def _():
            last_forward(k - OWN).wait_send()

        arrived(gath.at[k, far, 0:mid], half_recv.at[b, 0])
        arrived(gath.at[k, far, mid:high], half_recv.at[b, 1])
        last_forward(k).start()

    def down_loads(k, b):
        return [
            pltpu.make_async_copy(gath.at[k, :, tall : tall + ROWS], wd_b.at[b, :, :, 0 : 2 * wide], load_sem.at[b, 0]),
            pltpu.make_async_copy(gath.at[k, :, tall + ROWS : high], wd_b.at[b, :, :, 2 * wide : 4 * wide], load_sem.at[b, 1]),
        ]

    def loads(k):
        b = lax.rem(k, 2)
        return [pltpu.make_async_copy(gath.at[k, :, 0:tall], wgu_b.at[b], load_sem.at[b, 2])] + down_loads(k, b)

    def e4(k):
        b = lax.rem(k, OWN)
        other = 1 - 2 * c
        own_here(k).wait()
        for i, j in enumerate((me, left, right, far)):
            arrived(gath.at[k, j + other], part_recv.at[b, i])
        for copy in loads(k):
            copy.start()

    def pair_copy(r):
        b = lax.rem(r, 2)
        return remote(term.at[b, 1 - c], pair.at[b], pair_send.at[b], pair_recv.at[b], partner)

    def b_copies(r):
        b = lax.rem(r, DEEP)
        return [
            remote(part.at[b, 1, 0:mid], halves.at[b, 0], b_send.at[b, 0], b_recv.at[b, 0], right),
            remote(part.at[b, 1, mid:high], halves.at[b, 1], b_send.at[b, 1], b_recv.at[b, 1], left),
        ]

    def c_copies(r):
        b = lax.rem(r, DEEP)
        return [
            remote(part.at[b, 0], wholes.at[b, 0], c_send.at[b, 0], c_recv.at[b, 0], right),
            remote(part.at[b, 2], wholes.at[b, 1], c_send.at[b, 1], c_recv.at[b, 1], left),
        ]

    def free(sem, to):
        pl.semaphore_signal(sem, inc=1, device_id={"dp": to}, device_id_type=MESH)

    STRIP = 48

    def f1(r):
        @pl.when(r >= 2)
        def _():
            pl.semaphore_wait(pair_free, 1)

        pair_copy(r).start()

    def f2(r):
        b, p = lax.rem(r, DEEP), lax.rem(r, 2)

        @pl.when(r >= DEEP)
        def _():
            for copy in b_copies(r - DEEP) + c_copies(r - DEEP):
                copy.wait_send()
            pl.semaphore_wait(b_free.at[0], 1)
            pl.semaphore_wait(b_free.at[1], 1)

        pair_copy(r).wait_recv()
        for away, chip in ((2, over), (1, right_chip), (3, left_chip), (0, at)):
            for row in range(0, high, STRIP):
                total = term[p, c, chip, row : row + STRIP, :].astype(F32) + pair[p, chip, row : row + STRIP, :].astype(F32)
                if away:
                    part[b, away - 1, row : row + STRIP, :] = total.astype(BF16)
                else:
                    fin[b, row : row + STRIP, :] = total
        for copy in b_copies(r):
            copy.start()
        pair_copy(r).wait_send()

        @pl.when(r + 2 < chunks)
        def _():
            free(pair_free, partner)

    def f3(r):
        b = lax.rem(r, DEEP)

        @pl.when(r >= DEEP)
        def _():
            pl.semaphore_wait(c_free.at[0], 1)
            pl.semaphore_wait(c_free.at[1], 1)

        for i in range(2):
            b_copies(r)[i].wait_recv()
            start = mid * i
            for row in range(0, mid, STRIP):
                total = part[b, 2 * i, start + row : start + row + STRIP, :].astype(F32) + halves[b, i, row : row + STRIP, :].astype(F32)
                part[b, 2 * i, start + row : start + row + STRIP, :] = total.astype(BF16)

        @pl.when(r + DEEP < chunks)
        def _():
            free(b_free.at[0], left)
            free(b_free.at[1], right)

        for copy in c_copies(r):
            copy.start()

    def f4(r):
        b = lax.rem(r, DEEP)
        layer, s = 1 - lax.div(r, slots), lax.rem(r, slots)
        for copy in c_copies(r):
            copy.wait_recv()
        lanes = lax.broadcasted_iota(jnp.int32, (tall, 128), 1) // ROWS
        out = squares[...]
        for half, grad in ((0, gg), (1, gu)):
            for group in range(n // 4):
                cols = slice(half * wide + 128 * group, half * wide + 128 * (group + 1))
                total = fin[b, 0:tall, cols] + wholes[b, 0, 0:tall, cols].astype(F32) + wholes[b, 1, 0:tall, cols].astype(F32)
                total = total.astype(BF16).astype(F32)
                out = out + jnp.sum((total * total).reshape(tall // 8, 8, 128), axis=0)
                for place in range(4):
                    unit = slots * (4 * group + place) + s
                    where = pl.ds(pl.multiple_of(lax.div(unit, 4) * 128, 128), 128)
                    moved = pltpu.roll(total, lax.rem(lax.rem(unit, 4) + 4 - place, 4) * ROWS, 1)
                    grad[layer, :, where] = jnp.where(lanes == lax.rem(unit, 4), moved, grad[layer, :, where].astype(F32)).astype(BF16)
        for half in range(2):
            rows = slice(tall + ROWS * half, tall + ROWS * (half + 1))
            total = fin[b, rows, :] + wholes[b, 0, rows, :].astype(F32) + wholes[b, 1, rows, :].astype(F32)
            total = total.astype(BF16).astype(F32)
            gd[layer, pl.ds(pl.multiple_of(s * ROWS, ROWS), ROWS), 2 * wide * half : 2 * wide * (half + 1)] = total.astype(BF16)
            for lane in range(0, 2 * wide, 128):
                one = total[:, lane : lane + 128]
                out = out + jnp.sum((one * one).reshape(ROWS // 8, 8, 128), axis=0)
        squares[...] = out

        @pl.when(r + DEEP < chunks)
        def _():
            free(c_free.at[0], left)
            free(c_free.at[1], right)

    def turn(block, dst, start, size):
        for q in range(0, d, 256):
            dst[q : q + 256, pl.ds(start, size)] = block[:, q : q + 256].T.astype(BF16)

    def gates(rows, b):
        both = dot(va[rows, :], wgu_b[b].reshape(d, 2 * wide))
        g, u = both[:, :wide], both[:, wide:]
        sig = jax.nn.sigmoid(g)
        silu = g * sig
        return silu, u * (sig + silu * (1.0 - sig)), (silu * u).astype(BF16)

    def gradients(r, a):
        p = lax.rem(r, 2)
        for m in range(2):
            g = dot(vat[512 * m : 512 * (m + 1), :], dgu[...]).astype(BF16)
            for i in range(512 // tall):
                j = m * (512 // tall) + i
                term[p, j % 2, j // 2, 0:tall, :] = g[tall * i : tall * (i + 1), :]
        hidden = act[a]
        for m in range(4):
            g = dot(vct[256 * m : 256 * (m + 1), :], hidden).T.astype(BF16)
            low = tall + ROWS * (m // 2)
            for j in range(n):
                term[p, j % 2, j // 2, low : low + ROWS, 256 * (m % 2) : 256 * (m % 2 + 1)] = g[ROWS * j : ROWS * (j + 1), :]

    def stashes(t, b):
        return [
            pltpu.make_async_copy(act.at[b], act_st.at[t], stash_sem.at[b, 0]),
            pltpu.make_async_copy(sgu.at[b], sgu_st.at[t], stash_sem.at[b, 1]),
        ]

    def saved(s):
        b = lax.rem(s, 2)
        return down_loads(s, b) + [
            pltpu.make_async_copy(act_st.at[s], act.at[b], saved_sem.at[b, 0]),
            pltpu.make_async_copy(sgu_st.at[s], sgu.at[b], saved_sem.at[b, 1]),
        ]

    x_in = pltpu.make_async_copy(x, va, in_sem.at[0])
    dy_in = pltpu.make_async_copy(dy, vc, in_sem.at[1])
    x_in.start()
    dy_in.start()
    barrier = pltpu.get_barrier_semaphore()
    for i in range(1, n):
        pl.semaphore_signal(barrier, inc=1, device_id={"dp": lax.rem(me + i, n)}, device_id_type=MESH)
    prepare(0)
    pl.semaphore_wait(barrier, n - 1)
    e1(0)
    e1(1)
    x_in.wait()

    def first(i, _):
        start = pl.multiple_of(i * 256, 256)
        rows = pl.ds(start, 256)
        h = va[rows, :].astype(F32)
        a = (h * lax.rsqrt(jnp.mean(h * h, -1, keepdims=True) + 1e-6)).astype(BF16)
        va[rows, :] = a
        turn(a.astype(F32), vat, start, 256)
        acc[rows, :] = jnp.zeros((256, d), F32)
        return 0

    lax.fori_loop(0, tokens // 256, first, 0)
    a0t_out = pltpu.make_async_copy(vat, a0t_st, in_sem.at[2])
    a0t_out.start()
    e2(0)
    e1(2)
    dy_in.wait()

    def second(i, _):
        start = pl.multiple_of(i * 256, 256)
        turn(vc[pl.ds(start, 256), :].astype(F32), vct, start, 256)
        return 0

    lax.fori_loop(0, tokens // 256, second, 0)
    e3(0)
    e2(1)
    e4(0)
    gg[...] = jnp.zeros_like(gg)
    gu[...] = jnp.zeros_like(gu)
    squares[...] = jnp.zeros_like(squares)

    def forward(t, _):
        e1(t + 3)
        e3(t + 1)
        for copy in loads(t):
            copy.wait()
        b = lax.rem(t, 2)

        @pl.when(t >= 2)
        def _():
            for copy in stashes(t - 2, b):
                copy.wait()

        def work(i, _):
            rows = pl.ds(pl.multiple_of(i * BLOCK, BLOCK), BLOCK)
            silu, slope, hidden = gates(rows, b)
            act[b, rows, :] = hidden
            sgu[b, rows, 0:wide] = slope
            sgu[b, rows, wide:] = silu
            acc[rows, :] += dot(hidden, wd_b[b].reshape(n * ROWS, d))
            return 0

        lax.fori_loop(0, blocks // 2, work, 0)
        e2(t + 2)
        e4(t + 1)
        lax.fori_loop(blocks // 2, blocks, work, 0)
        for copy in stashes(t, b):
            copy.start()
        return 0

    lax.fori_loop(0, slots, forward, 0)
    x_in.start()
    a0t_out.wait()
    for t in (slots - 2, slots - 1):
        for copy in stashes(t, t % 2):
            copy.wait()
    x_in.wait()

    def between(i, _):
        start = pl.multiple_of(i * 256, 256)
        rows = pl.ds(start, 256)
        h = (va[rows, :].astype(F32) + acc[rows, :].astype(BF16).astype(F32)).astype(BF16).astype(F32)
        sgu[0, rows, :] = h[:, : 2 * wide]
        sgu[1, rows, :] = h[:, 2 * wide :]
        a = (h * lax.rsqrt(jnp.mean(h * h, -1, keepdims=True) + 1e-6)).astype(BF16)
        va[rows, :] = a
        turn(a.astype(F32), vat, start, 256)
        acc[rows, :] = jnp.zeros((256, d), F32)
        return 0

    lax.fori_loop(0, tokens // 256, between, 0)

    def both_ways(t, _):
        r = t - slots

        @pl.when(t + 3 < chunks)
        def _():
            e1(t + 3)

        @pl.when(t + 1 < chunks)
        def _():
            e3(t + 1)

        for copy in loads(t):
            copy.wait()
        b = lax.rem(t, 2)

        def work(i, _):
            rows = pl.ds(pl.multiple_of(i * BLOCK, BLOCK), BLOCK)
            silu, slope, hidden = gates(rows, b)
            by = dot_t(vc[rows, :], wd_b[b].reshape(n * ROWS, d)).astype(BF16).astype(F32)
            act[0, rows, :] = hidden
            dg, du = (by * slope).astype(BF16), (by * silu).astype(BF16)
            dgu[rows, 0:wide] = dg
            dgu[rows, wide:] = du
            acc[rows, :] += dot_t(jnp.concatenate([dg, du], axis=1), wgu_b[b].reshape(d, 2 * wide))
            return 0

        lax.fori_loop(0, blocks, work, 0)

        @pl.when(r >= 1)
        def _():
            f2(r - 1)

        @pl.when(r >= 2)
        def _():
            f3(r - 2)

        @pl.when(t + 2 < chunks)
        def _():
            e2(t + 2)

        @pl.when(t + 1 < chunks)
        def _():
            e4(t + 1)

        @pl.when(r >= 3)
        def _():
            f4(r - 3)

        gradients(r, 0)
        f1(r)
        return 0

    lax.fori_loop(slots, chunks, both_ways, 0)
    a0t_in = pltpu.make_async_copy(a0t_st, vat, in_sem.at[2])
    a0t_in.start()

    def back(i, _):
        start = pl.multiple_of(i * 256, 256)
        rows = pl.ds(start, 256)
        h = jnp.concatenate([sgu[0, rows, :], sgu[1, rows, :]], axis=1)
        da = acc[rows, :].astype(BF16).astype(F32)
        scale = lax.rsqrt(jnp.mean(h * h, -1, keepdims=True) + 1e-6)
        along = jnp.mean(da * h, -1, keepdims=True)
        by_h = (da * scale - h * (scale * scale * scale * along)).astype(BF16).astype(F32)
        by_h = (vc[rows, :].astype(F32) + by_h).astype(BF16)
        vc[rows, :] = by_h
        turn(by_h.astype(F32), vct, start, 256)
        return 0

    lax.fori_loop(0, tokens // 256, back, 0)
    for copy in saved(0):
        copy.start()
    a0t_in.wait()

    def backward(t, _):
        r, s = t - slots, t - chunks
        b = lax.rem(s, 2)
        for copy in saved(s):
            copy.wait()

        @pl.when(s + 1 < slots)
        def _():
            for copy in saved(s + 1):
                copy.start()

        def work(i, _):
            rows = pl.ds(pl.multiple_of(i * BLOCK, BLOCK), BLOCK)
            by = dot_t(vc[rows, :], wd_b[b].reshape(n * ROWS, d)).astype(BF16).astype(F32)
            dgu[rows, 0:wide] = (by * sgu[b, rows, 0:wide]).astype(BF16)
            dgu[rows, wide:] = (by * sgu[b, rows, wide:]).astype(BF16)
            return 0

        lax.fori_loop(0, blocks, work, 0)
        f2(r - 1)
        f3(r - 2)
        f4(r - 3)
        gradients(r, b)
        f1(r)
        return 0

    lax.fori_loop(chunks, chunks + slots, backward, 0)

    f2(chunks - 1)
    f3(chunks - 2)
    f4(chunks - 3)
    f3(chunks - 1)
    f4(chunks - 2)
    f4(chunks - 1)
    for k in range(chunks - OWN, chunks):
        for copy in own_copies(k) + forwards(k) + [last_forward(k)]:
            copy.wait_send()
    for r in range(chunks - DEEP, chunks):
        for copy in b_copies(r) + c_copies(r):
            copy.wait_send()

    norms[me] = squares[...]
    sends = [
        remote(squares, norms.at[me], norm_send.at[i], norm_recv.at[i], lax.rem(me + i + 1, n)) for i in range(n - 1)
    ]
    for copy in sends:
        copy.start()
    for i in range(n - 1):
        source = lax.rem(me + n - i - 1, n)
        remote(norms.at[source], norms.at[source], norm_send.at[i], norm_recv.at[i], me).wait_recv()
    for copy in sends:
        copy.wait_send()
    total = jnp.sum(norms[...])
    fac[...] = jnp.minimum(1.0, 0.5 * lax.rsqrt(jnp.full(fac.shape, total / count, F32) + 1e-30))


def gradients_of(n, x, dy, wg, wu, wd):
    layers, tall, ff = wg.shape
    down, d = wd.shape[1:]
    tokens = x.shape[0]
    slots, wide = down // ROWS, n * ROWS
    chunks, high = layers * slots, tall + 2 * ROWS
    chips = n // 2
    assert layers == 2 and chips == 4 and d == 4 * wide and tokens % BLOCK == 0 and down % ROWS == 0
    hbm, vmem = pl.BlockSpec(memory_space=pl.ANY), pl.BlockSpec(memory_space=pltpu.VMEM)
    dma, plain = pltpu.SemaphoreType.DMA, pltpu.SemaphoreType.REGULAR
    out = pl.pallas_call(
        functools.partial(kernel, n, float(n * (wg.size + wu.size + wd.size))),
        out_shape=(
            jax.ShapeDtypeStruct((chunks, n, high, 2 * wide), BF16),
            jax.ShapeDtypeStruct((slots, tokens, wide), BF16),
            jax.ShapeDtypeStruct((slots, tokens, 2 * wide), F32),
            jax.ShapeDtypeStruct((d, tokens), BF16),
            jax.ShapeDtypeStruct(wg.shape, BF16),
            jax.ShapeDtypeStruct(wu.shape, BF16),
            jax.ShapeDtypeStruct(wd.shape, BF16),
            jax.ShapeDtypeStruct((8, 128), F32),
        ),
        in_specs=[hbm, hbm, vmem, vmem, vmem],
        out_specs=(hbm, hbm, hbm, hbm, vmem, vmem, vmem, vmem),
        scratch_shapes=[
            pltpu.VMEM((tokens, d), BF16),
            pltpu.VMEM((d, tokens), BF16),
            pltpu.VMEM((tokens, d), BF16),
            pltpu.VMEM((d, tokens), BF16),
            pltpu.VMEM((tokens, d), F32),
            pltpu.VMEM((2, tokens, wide), BF16),
            pltpu.VMEM((2, tokens, 2 * wide), F32),
            pltpu.VMEM((tokens, 2 * wide), BF16),
            pltpu.VMEM((2, n, tall, 2 * wide), BF16),
            pltpu.VMEM((2, n, ROWS, d), BF16),
            pltpu.VMEM((OWN, high, 2 * wide), BF16),
            pltpu.VMEM((2, 2, chips, high, 2 * wide), BF16),
            pltpu.VMEM((2, chips, high, 2 * wide), BF16),
            pltpu.VMEM((DEEP, 3, high, 2 * wide), BF16),
            pltpu.VMEM((DEEP, high, 2 * wide), F32),
            pltpu.VMEM((DEEP, 2, high // 2, 2 * wide), BF16),
            pltpu.VMEM((DEEP, 2, high, 2 * wide), BF16),
            pltpu.VMEM((8, 128), F32),
            pltpu.VMEM((n, 8, 128), F32),
            dma((3,)),
            dma((OWN, 3)),
            dma((OWN,)),
            dma((OWN, 2)),
            dma((OWN, 2)),
            dma((OWN, 4)),
            dma((OWN, 5)),
            dma((2, 3)),
            dma((2, 2)),
            dma((2, 2)),
            dma((2,)),
            dma((2,)),
            dma((DEEP, 2)),
            dma((DEEP, 2)),
            dma((DEEP, 2)),
            dma((DEEP, 2)),
            dma((n - 1,)),
            dma((n - 1,)),
            plain,
            plain((2,)),
            plain((2,)),
        ],
        compiler_params=pltpu.CompilerParams(collective_id=0, has_side_effects=True, vmem_limit_bytes=67043328),
        cost_estimate=pl.CostEstimate(
            flops=30 * tokens * d * ff, bytes_accessed=200_000_000, transcendentals=2 * layers * tokens * ff
        ),
    )(x, dy, wg, wu, wd)
    return out[4:7], out[7][0, 0]


def adamw(w, m, v, g):
    m = 0.9 * m + 0.1 * g
    v = 0.95 * v + 0.05 * g * g
    step = m * lax.rsqrt(v + 1e-8) + 0.1 * w
    return (w - 0.02 * step).astype(BF16), m, v


def solution(mesh):
    n = mesh.shape["dp"]

    def step(x, dy, *arrays):
        weights, m, v = (arrays[i : i + 3] for i in (0, 3, 6))
        gradients, factor = gradients_of(n, x[0], dy[0], *weights)
        new = [
            adamw(w.astype(F32), m, v, g.astype(F32) * factor) for w, m, v, g in zip(weights, m, v, gradients, strict=True)
        ]
        return tuple(one[which] for which in range(3) for one in new)

    states, cut = P(("rep", "dp"), None, None), P(None, "dp", None)
    return jax.shard_map(
        step,
        mesh=mesh,
        in_specs=(states, states) + (cut,) * 9,
        out_specs=(P("rep", "dp", None),) * 9,
        check_vma=False,
    )
```

```python
import functools

import jax
import jax.numpy as jnp
from jax import lax
from jax.experimental import pallas as pl
from jax.experimental.pallas import tpu as pltpu
from jax.sharding import PartitionSpec as P

MESH = pl.DeviceIdType.MESH
F32, BF16 = jnp.float32, jnp.bfloat16
ROWS = 32
BLOCK = 512
OWN, DEEP = 6, 3


def dot(a, b):
    return lax.dot_general(a, b, (((1,), (0,)), ((), ())), preferred_element_type=F32)


def dot_t(a, b):
    return lax.dot_general(a, b, (((1,), (1,)), ((), ())), preferred_element_type=F32)


def kernel(
    n, count,
    x, dy, wg, wu, wd,
    gath, act_st, sgu_st, a0t_st, gg, gu, gd, fac,
    va, vat, vc, vct, acc, act, sgu, dgu, wgu_b, wd_b,
    own, term, pair, part, fin, halves, wholes, squares, norms,
    in_sem, own_send, own_local, full_recv, half_recv, part_recv, fwd_send, load_sem, stash_sem, saved_sem,
    pair_send, pair_recv, b_send, b_recv, c_send, c_recv, norm_send, norm_recv,
    pair_free, b_free, c_free,
):
    me = lax.axis_index("dp")
    chips = n // 2
    c, at = lax.rem(me, 2), lax.div(me, 2)
    over = lax.rem(at + 2, chips)
    right_chip, left_chip = lax.rem(at + 1, chips), lax.rem(at + chips - 1, chips)
    partner = at * 2 + 1 - c
    right, left, far = right_chip * 2 + c, left_chip * 2 + c, over * 2 + c
    tokens, d = va.shape
    wide = wgu_b.shape[3] // 2
    slots = wd.shape[1] // ROWS
    layers = wd.shape[0]
    chunks = layers * slots
    blocks = tokens // BLOCK
    high = own.shape[1]
    mid = high // 2
    tall = wg.shape[1]

    def remote(src, dst, send, recv, to):
        return pltpu.make_async_remote_copy(
            src_ref=src, dst_ref=dst, send_sem=send, recv_sem=recv, device_id={"dp": to}, device_id_type=MESH
        )

    def prepare(k):
        b, layer, s = lax.rem(k, OWN), lax.div(k, slots), lax.rem(k, slots)
        lanes = lax.broadcasted_iota(jnp.int32, (tall, 128), 1) // ROWS
        for w, base in ((wg, 0), (wu, wide)):
            for group in range(n // 4):
                total = None
                for place in range(4):
                    unit = slots * (4 * group + place) + s
                    piece = w[layer, :, pl.ds(pl.multiple_of(lax.div(unit, 4) * 128, 128), 128)].astype(F32)
                    piece = pltpu.roll(piece, lax.rem(place + 4 - lax.rem(unit, 4), 4) * ROWS, 1)
                    total = piece if total is None else jnp.where(lanes == place, piece, total)
                own[b, 0:tall, base + 128 * group : base + 128 * (group + 1)] = total.astype(BF16)
        rows = wd[layer, pl.ds(pl.multiple_of(s * ROWS, ROWS), ROWS), :]
        own[b, tall : tall + ROWS, :] = rows[:, : 2 * wide]
        own[b, tall + ROWS : high, :] = rows[:, 2 * wide :]

    def own_copies(k):
        b = lax.rem(k, OWN)
        return [
            remote(own.at[b], gath.at[k, me], own_send.at[b, 0], full_recv.at[b, 0], right),
            remote(own.at[b], gath.at[k, me], own_send.at[b, 1], full_recv.at[b, 1], left),
            remote(own.at[b], gath.at[k, me], own_send.at[b, 2], part_recv.at[b, 0], partner),
        ]

    def own_here(k):
        b = lax.rem(k, OWN)
        return pltpu.make_async_copy(own.at[b], gath.at[k, me], own_local.at[b])

    def e1(k):
        for copy in own_copies(k):
            copy.start()
        own_here(k).start()

        @pl.when(k + 1 < chunks)
        def _():
            @pl.when(k + 1 >= OWN)
            def _():
                for copy in own_copies(k + 1 - OWN):
                    copy.wait_send()

            prepare(k + 1)

    def arrived(region, recv):
        remote(region, region, fwd_send.at[0, 0], recv, me).wait_recv()

    def forwards(k):
        b = lax.rem(k, OWN)
        return [
            remote(gath.at[k, left, 0:mid], gath.at[k, left, 0:mid], fwd_send.at[b, 0], half_recv.at[b, 0], right),
            remote(gath.at[k, right, mid:high], gath.at[k, right, mid:high], fwd_send.at[b, 1], half_recv.at[b, 1], left),
            remote(gath.at[k, left], gath.at[k, left], fwd_send.at[b, 2], part_recv.at[b, 1], partner),
            remote(gath.at[k, right], gath.at[k, right], fwd_send.at[b, 3], part_recv.at[b, 2], partner),
        ]

    def last_forward(k):
        b = lax.rem(k, OWN)
        return remote(gath.at[k, far], gath.at[k, far], fwd_send.at[b, 4], part_recv.at[b, 3], partner)

    def e2(k):
        b = lax.rem(k, OWN)

        @pl.when(k >= OWN)
        def _():
            for copy in forwards(k - OWN):
                copy.wait_send()

        arrived(gath.at[k, left], full_recv.at[b, 0])
        arrived(gath.at[k, right], full_recv.at[b, 1])
        for copy in forwards(k):
            copy.start()

    def e3(k):
        b = lax.rem(k, OWN)

        @pl.when(k >= OWN)
        def _():
            last_forward(k - OWN).wait_send()

        arrived(gath.at[k, far, 0:mid], half_recv.at[b, 0])
        arrived(gath.at[k, far, mid:high], half_recv.at[b, 1])
        last_forward(k).start()

    def down_loads(k, b):
        return [
            pltpu.make_async_copy(gath.at[k, :, tall : tall + ROWS], wd_b.at[b, :, :, 0 : 2 * wide], load_sem.at[b, 0]),
            pltpu.make_async_copy(gath.at[k, :, tall + ROWS : high], wd_b.at[b, :, :, 2 * wide : 4 * wide], load_sem.at[b, 1]),
        ]

    def loads(k):
        b = lax.rem(k, 2)
        return [pltpu.make_async_copy(gath.at[k, :, 0:tall], wgu_b.at[b], load_sem.at[b, 2])] + down_loads(k, b)

    def e4(k):
        b = lax.rem(k, OWN)
        other = 1 - 2 * c
        own_here(k).wait()
        for i, j in enumerate((me, left, right, far)):
            arrived(gath.at[k, j + other], part_recv.at[b, i])
        for copy in loads(k):
            copy.start()

    def pair_copy(r):
        b = lax.rem(r, 2)
        return remote(term.at[b, 1 - c], pair.at[b], pair_send.at[b], pair_recv.at[b], partner)

    def b_copies(r):
        b = lax.rem(r, DEEP)
        return [
            remote(part.at[b, 1, 0:mid], halves.at[b, 0], b_send.at[b, 0], b_recv.at[b, 0], right),
            remote(part.at[b, 1, mid:high], halves.at[b, 1], b_send.at[b, 1], b_recv.at[b, 1], left),
        ]

    def c_copies(r):
        b = lax.rem(r, DEEP)
        return [
            remote(part.at[b, 0], wholes.at[b, 0], c_send.at[b, 0], c_recv.at[b, 0], right),
            remote(part.at[b, 2], wholes.at[b, 1], c_send.at[b, 1], c_recv.at[b, 1], left),
        ]

    def free(sem, to):
        pl.semaphore_signal(sem, inc=1, device_id={"dp": to}, device_id_type=MESH)

    STRIP = 48

    def f1(r):
        @pl.when(r >= 2)
        def _():
            pl.semaphore_wait(pair_free, 1)

        pair_copy(r).start()

    def f2(r):
        b, p = lax.rem(r, DEEP), lax.rem(r, 2)

        @pl.when(r >= DEEP)
        def _():
            for copy in b_copies(r - DEEP) + c_copies(r - DEEP):
                copy.wait_send()
            pl.semaphore_wait(b_free.at[0], 1)
            pl.semaphore_wait(b_free.at[1], 1)

        pair_copy(r).wait_recv()
        for away, chip in ((2, over), (1, right_chip), (3, left_chip), (0, at)):
            for row in range(0, high, STRIP):
                total = term[p, c, chip, row : row + STRIP, :].astype(F32) + pair[p, chip, row : row + STRIP, :].astype(F32)
                if away:
                    part[b, away - 1, row : row + STRIP, :] = total.astype(BF16)
                else:
                    fin[b, row : row + STRIP, :] = total
        for copy in b_copies(r):
            copy.start()
        pair_copy(r).wait_send()

        @pl.when(r + 2 < chunks)
        def _():
            free(pair_free, partner)

    def f3(r):
        b = lax.rem(r, DEEP)

        @pl.when(r >= DEEP)
        def _():
            pl.semaphore_wait(c_free.at[0], 1)
            pl.semaphore_wait(c_free.at[1], 1)

        for i in range(2):
            b_copies(r)[i].wait_recv()
            start = mid * i
            for row in range(0, mid, STRIP):
                total = part[b, 2 * i, start + row : start + row + STRIP, :].astype(F32) + halves[b, i, row : row + STRIP, :].astype(F32)
                part[b, 2 * i, start + row : start + row + STRIP, :] = total.astype(BF16)

        @pl.when(r + DEEP < chunks)
        def _():
            free(b_free.at[0], left)
            free(b_free.at[1], right)

        for copy in c_copies(r):
            copy.start()

    def f4(r):
        b = lax.rem(r, DEEP)
        layer, s = 1 - lax.div(r, slots), lax.rem(r, slots)
        for copy in c_copies(r):
            copy.wait_recv()
        lanes = lax.broadcasted_iota(jnp.int32, (tall, 128), 1) // ROWS
        out = squares[...]
        for half, grad in ((0, gg), (1, gu)):
            for group in range(n // 4):
                cols = slice(half * wide + 128 * group, half * wide + 128 * (group + 1))
                total = fin[b, 0:tall, cols] + wholes[b, 0, 0:tall, cols].astype(F32) + wholes[b, 1, 0:tall, cols].astype(F32)
                total = total.astype(BF16).astype(F32)
                out = out + jnp.sum((total * total).reshape(tall // 8, 8, 128), axis=0)
                for place in range(4):
                    unit = slots * (4 * group + place) + s
                    where = pl.ds(pl.multiple_of(lax.div(unit, 4) * 128, 128), 128)
                    moved = pltpu.roll(total, lax.rem(lax.rem(unit, 4) + 4 - place, 4) * ROWS, 1)
                    grad[layer, :, where] = jnp.where(lanes == lax.rem(unit, 4), moved, grad[layer, :, where].astype(F32)).astype(BF16)
        for half in range(2):
            rows = slice(tall + ROWS * half, tall + ROWS * (half + 1))
            total = fin[b, rows, :] + wholes[b, 0, rows, :].astype(F32) + wholes[b, 1, rows, :].astype(F32)
            total = total.astype(BF16).astype(F32)
            gd[layer, pl.ds(pl.multiple_of(s * ROWS, ROWS), ROWS), 2 * wide * half : 2 * wide * (half + 1)] = total.astype(BF16)
            for lane in range(0, 2 * wide, 128):
                one = total[:, lane : lane + 128]
                out = out + jnp.sum((one * one).reshape(ROWS // 8, 8, 128), axis=0)
        squares[...] = out

        @pl.when(r + DEEP < chunks)
        def _():
            free(c_free.at[0], left)
            free(c_free.at[1], right)

    def turn(block, dst, start, size):
        for q in range(0, d, 256):
            dst[q : q + 256, pl.ds(start, size)] = block[:, q : q + 256].T.astype(BF16)

    def gates(rows, b):
        both = dot(va[rows, :], wgu_b[b].reshape(d, 2 * wide))
        g, u = both[:, :wide], both[:, wide:]
        sig = jax.nn.sigmoid(g)
        silu = g * sig
        return silu, u * (sig + silu * (1.0 - sig)), (silu * u).astype(BF16)

    def gradients(r, a):
        p = lax.rem(r, 2)
        for m in range(2):
            g = dot(vat[512 * m : 512 * (m + 1), :], dgu[...]).astype(BF16)
            for i in range(512 // tall):
                j = m * (512 // tall) + i
                term[p, j % 2, j // 2, 0:tall, :] = g[tall * i : tall * (i + 1), :]
        hidden = act[a]
        for m in range(4):
            g = dot(vct[256 * m : 256 * (m + 1), :], hidden).T.astype(BF16)
            low = tall + ROWS * (m // 2)
            for j in range(n):
                term[p, j % 2, j // 2, low : low + ROWS, 256 * (m % 2) : 256 * (m % 2 + 1)] = g[ROWS * j : ROWS * (j + 1), :]

    def stashes(t, b):
        return [
            pltpu.make_async_copy(act.at[b], act_st.at[t], stash_sem.at[b, 0]),
            pltpu.make_async_copy(sgu.at[b], sgu_st.at[t], stash_sem.at[b, 1]),
        ]

    def saved(s):
        b = lax.rem(s, 2)
        return down_loads(s, b) + [
            pltpu.make_async_copy(act_st.at[s], act.at[b], saved_sem.at[b, 0]),
            pltpu.make_async_copy(sgu_st.at[s], sgu.at[b], saved_sem.at[b, 1]),
        ]

    x_in = pltpu.make_async_copy(x, va, in_sem.at[0])
    dy_in = pltpu.make_async_copy(dy, vc, in_sem.at[1])
    x_in.start()
    dy_in.start()
    barrier = pltpu.get_barrier_semaphore()
    for i in range(1, n):
        pl.semaphore_signal(barrier, inc=1, device_id={"dp": lax.rem(me + i, n)}, device_id_type=MESH)
    prepare(0)
    pl.semaphore_wait(barrier, n - 1)
    e1(0)
    e1(1)
    x_in.wait()

    def first(i, _):
        start = pl.multiple_of(i * 256, 256)
        rows = pl.ds(start, 256)
        h = va[rows, :].astype(F32)
        a = (h * lax.rsqrt(jnp.mean(h * h, -1, keepdims=True) + 1e-6)).astype(BF16)
        va[rows, :] = a
        turn(a.astype(F32), vat, start, 256)
        acc[rows, :] = jnp.zeros((256, d), F32)
        return 0

    lax.fori_loop(0, tokens // 256, first, 0)
    a0t_out = pltpu.make_async_copy(vat, a0t_st, in_sem.at[2])
    a0t_out.start()
    e2(0)
    e1(2)
    dy_in.wait()

    def second(i, _):
        start = pl.multiple_of(i * 256, 256)
        turn(vc[pl.ds(start, 256), :].astype(F32), vct, start, 256)
        return 0

    lax.fori_loop(0, tokens // 256, second, 0)
    e3(0)
    e2(1)
    e1(3)
    e4(0)
    gg[...] = jnp.zeros_like(gg)
    gu[...] = jnp.zeros_like(gu)
    squares[...] = jnp.zeros_like(squares)

    def forward(t, _):
        e2(t + 2)
        e3(t + 1)
        e1(t + 4)
        for copy in loads(t):
            copy.wait()
        b = lax.rem(t, 2)

        @pl.when(t >= 2)
        def _():
            for copy in stashes(t - 2, b):
                copy.wait()

        def work(i, _):
            rows = pl.ds(pl.multiple_of(i * BLOCK, BLOCK), BLOCK)
            silu, slope, hidden = gates(rows, b)
            act[b, rows, :] = hidden
            sgu[b, rows, 0:wide] = slope
            sgu[b, rows, wide:] = silu
            acc[rows, :] += dot(hidden, wd_b[b].reshape(n * ROWS, d))
            return 0

        lax.fori_loop(0, blocks // 2, work, 0)
        e4(t + 1)
        lax.fori_loop(blocks // 2, blocks, work, 0)
        for copy in stashes(t, b):
            copy.start()
        return 0

    lax.fori_loop(0, slots, forward, 0)
    x_in.start()
    a0t_out.wait()
    for t in (slots - 2, slots - 1):
        for copy in stashes(t, t % 2):
            copy.wait()
    x_in.wait()

    def between(i, _):
        start = pl.multiple_of(i * 256, 256)
        rows = pl.ds(start, 256)
        h = (va[rows, :].astype(F32) + acc[rows, :].astype(BF16).astype(F32)).astype(BF16).astype(F32)
        sgu[0, rows, :] = h[:, : 2 * wide]
        sgu[1, rows, :] = h[:, 2 * wide :]
        a = (h * lax.rsqrt(jnp.mean(h * h, -1, keepdims=True) + 1e-6)).astype(BF16)
        va[rows, :] = a
        turn(a.astype(F32), vat, start, 256)
        acc[rows, :] = jnp.zeros((256, d), F32)
        return 0

    lax.fori_loop(0, tokens // 256, between, 0)

    def both_ways(t, _):
        r = t - slots

        @pl.when(t + 2 < chunks)
        def _():
            e2(t + 2)

        @pl.when(t + 1 < chunks)
        def _():
            e3(t + 1)

        @pl.when(t + 4 < chunks)
        def _():
            e1(t + 4)

        for copy in loads(t):
            copy.wait()
        b = lax.rem(t, 2)

        def work(i, _):
            rows = pl.ds(pl.multiple_of(i * BLOCK, BLOCK), BLOCK)
            silu, slope, hidden = gates(rows, b)
            by = dot_t(vc[rows, :], wd_b[b].reshape(n * ROWS, d)).astype(BF16).astype(F32)
            act[0, rows, :] = hidden
            dg, du = (by * slope).astype(BF16), (by * silu).astype(BF16)
            dgu[rows, 0:wide] = dg
            dgu[rows, wide:] = du
            acc[rows, :] += dot_t(jnp.concatenate([dg, du], axis=1), wgu_b[b].reshape(d, 2 * wide))
            return 0

        lax.fori_loop(0, blocks, work, 0)

        @pl.when(t + 1 < chunks)
        def _():
            e4(t + 1)

        @pl.when(r >= 4)
        def _():
            f4(r - 4)

        @pl.when(r >= 1)
        def _():
            f2(r - 1)

        @pl.when(r >= 2)
        def _():
            f3(r - 2)

        gradients(r, 0)
        f1(r)
        return 0

    lax.fori_loop(slots, chunks, both_ways, 0)
    a0t_in = pltpu.make_async_copy(a0t_st, vat, in_sem.at[2])
    a0t_in.start()
    for copy in saved(0)[:3]:
        copy.start()

    def back(i, _):
        start = pl.multiple_of(i * 256, 256)
        rows = pl.ds(start, 256)
        h = jnp.concatenate([sgu[0, rows, :], sgu[1, rows, :]], axis=1)
        da = acc[rows, :].astype(BF16).astype(F32)
        scale = lax.rsqrt(jnp.mean(h * h, -1, keepdims=True) + 1e-6)
        along = jnp.mean(da * h, -1, keepdims=True)
        by_h = (da * scale - h * (scale * scale * scale * along)).astype(BF16).astype(F32)
        by_h = (vc[rows, :].astype(F32) + by_h).astype(BF16)
        vc[rows, :] = by_h
        turn(by_h.astype(F32), vct, start, 256)
        return 0

    lax.fori_loop(0, tokens // 256, back, 0)
    saved(0)[3].start()
    a0t_in.wait()

    def backward(t, _):
        r, s = t - slots, t - chunks
        b = lax.rem(s, 2)
        for copy in saved(s):
            copy.wait()

        @pl.when(s + 1 < slots)
        def _():
            for copy in saved(s + 1):
                copy.start()

        def work(i, _):
            rows = pl.ds(pl.multiple_of(i * BLOCK, BLOCK), BLOCK)
            by = dot_t(vc[rows, :], wd_b[b].reshape(n * ROWS, d)).astype(BF16).astype(F32)
            dgu[rows, 0:wide] = (by * sgu[b, rows, 0:wide]).astype(BF16)
            dgu[rows, wide:] = (by * sgu[b, rows, wide:]).astype(BF16)
            return 0

        lax.fori_loop(0, blocks, work, 0)
        f4(r - 4)
        f2(r - 1)
        f3(r - 2)
        gradients(r, b)
        f1(r)
        return 0

    lax.fori_loop(chunks, chunks + slots, backward, 0)

    f4(chunks - 4)
    f2(chunks - 1)
    f3(chunks - 2)
    f4(chunks - 3)
    f3(chunks - 1)
    f4(chunks - 2)
    f4(chunks - 1)
    for k in range(chunks - OWN, chunks):
        for copy in own_copies(k) + forwards(k) + [last_forward(k)]:
            copy.wait_send()
    for r in range(chunks - DEEP, chunks):
        for copy in b_copies(r) + c_copies(r):
            copy.wait_send()

    norms[me] = squares[...]
    sends = [
        remote(squares, norms.at[me], norm_send.at[i], norm_recv.at[i], lax.rem(me + i + 1, n)) for i in range(n - 1)
    ]
    for copy in sends:
        copy.start()
    for i in range(n - 1):
        source = lax.rem(me + n - i - 1, n)
        remote(norms.at[source], norms.at[source], norm_send.at[i], norm_recv.at[i], me).wait_recv()
    for copy in sends:
        copy.wait_send()
    total = jnp.sum(norms[...])
    fac[...] = jnp.minimum(1.0, 0.5 * lax.rsqrt(jnp.full(fac.shape, total / count, F32) + 1e-30))


def gradients_of(n, x, dy, wg, wu, wd):
    layers, tall, ff = wg.shape
    down, d = wd.shape[1:]
    tokens = x.shape[0]
    slots, wide = down // ROWS, n * ROWS
    chunks, high = layers * slots, tall + 2 * ROWS
    chips = n // 2
    assert layers == 2 and chips == 4 and d == 4 * wide and tokens % BLOCK == 0 and down % ROWS == 0
    hbm, vmem = pl.BlockSpec(memory_space=pl.ANY), pl.BlockSpec(memory_space=pltpu.VMEM)
    dma, plain = pltpu.SemaphoreType.DMA, pltpu.SemaphoreType.REGULAR
    out = pl.pallas_call(
        functools.partial(kernel, n, float(n * (wg.size + wu.size + wd.size))),
        out_shape=(
            jax.ShapeDtypeStruct((chunks, n, high, 2 * wide), BF16),
            jax.ShapeDtypeStruct((slots, tokens, wide), BF16),
            jax.ShapeDtypeStruct((slots, tokens, 2 * wide), F32),
            jax.ShapeDtypeStruct((d, tokens), BF16),
            jax.ShapeDtypeStruct(wg.shape, BF16),
            jax.ShapeDtypeStruct(wu.shape, BF16),
            jax.ShapeDtypeStruct(wd.shape, BF16),
            jax.ShapeDtypeStruct((8, 128), F32),
        ),
        in_specs=[hbm, hbm, vmem, vmem, vmem],
        out_specs=(hbm, hbm, hbm, hbm, vmem, vmem, vmem, vmem),
        scratch_shapes=[
            pltpu.VMEM((tokens, d), BF16),
            pltpu.VMEM((d, tokens), BF16),
            pltpu.VMEM((tokens, d), BF16),
            pltpu.VMEM((d, tokens), BF16),
            pltpu.VMEM((tokens, d), F32),
            pltpu.VMEM((2, tokens, wide), BF16),
            pltpu.VMEM((2, tokens, 2 * wide), F32),
            pltpu.VMEM((tokens, 2 * wide), BF16),
            pltpu.VMEM((2, n, tall, 2 * wide), BF16),
            pltpu.VMEM((2, n, ROWS, d), BF16),
            pltpu.VMEM((OWN, high, 2 * wide), BF16),
            pltpu.VMEM((2, 2, chips, high, 2 * wide), BF16),
            pltpu.VMEM((2, chips, high, 2 * wide), BF16),
            pltpu.VMEM((DEEP, 3, high, 2 * wide), BF16),
            pltpu.VMEM((DEEP, high, 2 * wide), F32),
            pltpu.VMEM((DEEP, 2, high // 2, 2 * wide), BF16),
            pltpu.VMEM((DEEP, 2, high, 2 * wide), BF16),
            pltpu.VMEM((8, 128), F32),
            pltpu.VMEM((n, 8, 128), F32),
            dma((3,)),
            dma((OWN, 3)),
            dma((OWN,)),
            dma((OWN, 2)),
            dma((OWN, 2)),
            dma((OWN, 4)),
            dma((OWN, 5)),
            dma((2, 3)),
            dma((2, 2)),
            dma((2, 2)),
            dma((2,)),
            dma((2,)),
            dma((DEEP, 2)),
            dma((DEEP, 2)),
            dma((DEEP, 2)),
            dma((DEEP, 2)),
            dma((n - 1,)),
            dma((n - 1,)),
            plain,
            plain((2,)),
            plain((2,)),
        ],
        compiler_params=pltpu.CompilerParams(collective_id=0, has_side_effects=True, vmem_limit_bytes=67043328),
        cost_estimate=pl.CostEstimate(
            flops=30 * tokens * d * ff, bytes_accessed=200_000_000, transcendentals=2 * layers * tokens * ff
        ),
    )(x, dy, wg, wu, wd)
    return out[4:7], out[7][0, 0]


def adamw(w, m, v, g):
    m = 0.9 * m + 0.1 * g
    v = 0.95 * v + 0.05 * g * g
    step = m * lax.rsqrt(v + 1e-8) + 0.1 * w
    return (w - 0.02 * step).astype(BF16), m, v


def solution(mesh):
    n = mesh.shape["dp"]

    def step(x, dy, *arrays):
        weights, m, v = (arrays[i : i + 3] for i in (0, 3, 6))
        gradients, factor = gradients_of(n, x[0], dy[0], *weights)
        new = [
            adamw(w.astype(F32), m, v, g.astype(F32) * factor) for w, m, v, g in zip(weights, m, v, gradients, strict=True)
        ]
        return tuple(one[which] for which in range(3) for one in new)

    states, cut = P(("rep", "dp"), None, None), P(None, "dp", None)
    return jax.shard_map(
        step,
        mesh=mesh,
        in_specs=(states, states) + (cut,) * 9,
        out_specs=(P("rep", "dp", None),) * 9,
        check_vma=False,
    )
```

```python
import functools

import jax
import jax.numpy as jnp
from jax import lax
from jax.experimental import pallas as pl
from jax.experimental.pallas import tpu as pltpu
from jax.sharding import PartitionSpec as P

MESH = pl.DeviceIdType.MESH
F32, BF16 = jnp.float32, jnp.bfloat16
ROWS = 32
BLOCK = 512
OWN, DEEP = 6, 3


def dot(a, b):
    return lax.dot_general(a, b, (((1,), (0,)), ((), ())), preferred_element_type=F32)


def dot_t(a, b):
    return lax.dot_general(a, b, (((1,), (1,)), ((), ())), preferred_element_type=F32)


def kernel(
    n, count,
    x, dy, wg, wu, wd,
    gath, act_st, sgu_st, a0t_st, gg, gu, gd, fac,
    va, vat, vc, vct, acc, act, sgu, dgu, wgu_b, wd_b,
    own, term, pair, part, fin, halves, wholes, squares, norms,
    in_sem, own_send, own_local, full_recv, half_recv, part_recv, fwd_send, load_sem, stash_sem, saved_sem,
    pair_send, pair_recv, b_send, b_recv, c_send, c_recv, norm_send, norm_recv,
    pair_free, b_free, c_free,
):
    me = lax.axis_index("dp")
    chips = n // 2
    c, at = lax.rem(me, 2), lax.div(me, 2)
    over = lax.rem(at + 2, chips)
    right_chip, left_chip = lax.rem(at + 1, chips), lax.rem(at + chips - 1, chips)
    partner = at * 2 + 1 - c
    right, left, far = right_chip * 2 + c, left_chip * 2 + c, over * 2 + c
    tokens, d = va.shape
    wide = wgu_b.shape[3] // 2
    slots = wd.shape[1] // ROWS
    layers = wd.shape[0]
    chunks = layers * slots
    blocks = tokens // BLOCK
    high = own.shape[1]
    mid = high // 2
    tall = wg.shape[1]

    def remote(src, dst, send, recv, to):
        return pltpu.make_async_remote_copy(
            src_ref=src, dst_ref=dst, send_sem=send, recv_sem=recv, device_id={"dp": to}, device_id_type=MESH
        )

    def prepare(k):
        b, layer, s = lax.rem(k, OWN), lax.div(k, slots), lax.rem(k, slots)
        lanes = lax.broadcasted_iota(jnp.int32, (tall, 128), 1) // ROWS
        for w, base in ((wg, 0), (wu, wide)):
            for group in range(n // 4):
                total = None
                for place in range(4):
                    unit = slots * (4 * group + place) + s
                    piece = w[layer, :, pl.ds(pl.multiple_of(lax.div(unit, 4) * 128, 128), 128)].astype(F32)
                    piece = pltpu.roll(piece, lax.rem(place + 4 - lax.rem(unit, 4), 4) * ROWS, 1)
                    total = piece if total is None else jnp.where(lanes == place, piece, total)
                own[b, 0:tall, base + 128 * group : base + 128 * (group + 1)] = total.astype(BF16)
        rows = wd[layer, pl.ds(pl.multiple_of(s * ROWS, ROWS), ROWS), :]
        own[b, tall : tall + ROWS, :] = rows[:, : 2 * wide]
        own[b, tall + ROWS : high, :] = rows[:, 2 * wide :]

    def own_copies(k):
        b = lax.rem(k, OWN)
        return [
            remote(own.at[b], gath.at[k, me], own_send.at[b, 0], full_recv.at[b, 0], right),
            remote(own.at[b], gath.at[k, me], own_send.at[b, 1], full_recv.at[b, 1], left),
            remote(own.at[b], gath.at[k, me], own_send.at[b, 2], part_recv.at[b, 0], partner),
        ]

    def own_here(k):
        b = lax.rem(k, OWN)
        return pltpu.make_async_copy(own.at[b], gath.at[k, me], own_local.at[b])

    def e1(k):
        for copy in own_copies(k):
            copy.start()
        own_here(k).start()

        @pl.when(k + 1 < chunks)
        def _():
            @pl.when(k + 1 >= OWN)
            def _():
                for copy in own_copies(k + 1 - OWN):
                    copy.wait_send()

            prepare(k + 1)

    def arrived(region, recv):
        remote(region, region, fwd_send.at[0, 0], recv, me).wait_recv()

    def forwards(k):
        b = lax.rem(k, OWN)
        return [
            remote(gath.at[k, left, 0:mid], gath.at[k, left, 0:mid], fwd_send.at[b, 0], half_recv.at[b, 0], right),
            remote(gath.at[k, right, mid:high], gath.at[k, right, mid:high], fwd_send.at[b, 1], half_recv.at[b, 1], left),
            remote(gath.at[k, left], gath.at[k, left], fwd_send.at[b, 2], part_recv.at[b, 1], partner),
            remote(gath.at[k, right], gath.at[k, right], fwd_send.at[b, 3], part_recv.at[b, 2], partner),
        ]

    def last_forward(k):
        b = lax.rem(k, OWN)
        return remote(gath.at[k, far], gath.at[k, far], fwd_send.at[b, 4], part_recv.at[b, 3], partner)

    def e2(k):
        b = lax.rem(k, OWN)

        @pl.when(k >= OWN)
        def _():
            for copy in forwards(k - OWN):
                copy.wait_send()

        arrived(gath.at[k, left], full_recv.at[b, 0])
        arrived(gath.at[k, right], full_recv.at[b, 1])
        for copy in forwards(k):
            copy.start()

    def e3(k):
        b = lax.rem(k, OWN)

        @pl.when(k >= OWN)
        def _():
            last_forward(k - OWN).wait_send()

        arrived(gath.at[k, far, 0:mid], half_recv.at[b, 0])
        arrived(gath.at[k, far, mid:high], half_recv.at[b, 1])
        last_forward(k).start()

    def down_loads(k, b):
        return [
            pltpu.make_async_copy(gath.at[k, :, tall : tall + ROWS], wd_b.at[b, :, :, 0 : 2 * wide], load_sem.at[b, 0]),
            pltpu.make_async_copy(gath.at[k, :, tall + ROWS : high], wd_b.at[b, :, :, 2 * wide : 4 * wide], load_sem.at[b, 1]),
        ]

    def loads(k):
        b = lax.rem(k, 2)
        return [pltpu.make_async_copy(gath.at[k, :, 0:tall], wgu_b.at[b], load_sem.at[b, 2])] + down_loads(k, b)

    def e4(k):
        b = lax.rem(k, OWN)
        other = 1 - 2 * c
        own_here(k).wait()
        for i, j in enumerate((me, left, right, far)):
            arrived(gath.at[k, j + other], part_recv.at[b, i])
        for copy in loads(k):
            copy.start()

    def pair_copy(r):
        b = lax.rem(r, 2)
        return remote(term.at[b, 1 - c], pair.at[b], pair_send.at[b], pair_recv.at[b], partner)

    def b_copies(r):
        b = lax.rem(r, DEEP)
        return [
            remote(part.at[b, 1, 0:mid], halves.at[b, 0], b_send.at[b, 0], b_recv.at[b, 0], right),
            remote(part.at[b, 1, mid:high], halves.at[b, 1], b_send.at[b, 1], b_recv.at[b, 1], left),
        ]

    def c_copies(r):
        b = lax.rem(r, DEEP)
        return [
            remote(part.at[b, 0], wholes.at[b, 0], c_send.at[b, 0], c_recv.at[b, 0], right),
            remote(part.at[b, 2], wholes.at[b, 1], c_send.at[b, 1], c_recv.at[b, 1], left),
        ]

    def free(sem, to):
        pl.semaphore_signal(sem, inc=1, device_id={"dp": to}, device_id_type=MESH)

    STRIP = 48

    def f1(r):
        @pl.when(r >= 2)
        def _():
            pl.semaphore_wait(pair_free, 1)

        pair_copy(r).start()

    def f2(r):
        b, p = lax.rem(r, DEEP), lax.rem(r, 2)

        @pl.when(r >= DEEP)
        def _():
            for copy in b_copies(r - DEEP) + c_copies(r - DEEP):
                copy.wait_send()
            pl.semaphore_wait(b_free.at[0], 1)
            pl.semaphore_wait(b_free.at[1], 1)

        pair_copy(r).wait_recv()
        for away, chip in ((2, over), (1, right_chip), (3, left_chip), (0, at)):
            for row in range(0, high, STRIP):
                total = term[p, c, chip, row : row + STRIP, :].astype(F32) + pair[p, chip, row : row + STRIP, :].astype(F32)
                if away:
                    part[b, away - 1, row : row + STRIP, :] = total.astype(BF16)
                else:
                    fin[b, row : row + STRIP, :] = total
        for copy in b_copies(r):
            copy.start()
        pair_copy(r).wait_send()

        @pl.when(r + 2 < chunks)
        def _():
            free(pair_free, partner)

    def f3(r):
        b = lax.rem(r, DEEP)

        @pl.when(r >= DEEP)
        def _():
            pl.semaphore_wait(c_free.at[0], 1)
            pl.semaphore_wait(c_free.at[1], 1)

        for i in range(2):
            b_copies(r)[i].wait_recv()
            start = mid * i
            for row in range(0, mid, STRIP):
                total = part[b, 2 * i, start + row : start + row + STRIP, :].astype(F32) + halves[b, i, row : row + STRIP, :].astype(F32)
                part[b, 2 * i, start + row : start + row + STRIP, :] = total.astype(BF16)

        @pl.when(r + DEEP < chunks)
        def _():
            free(b_free.at[0], left)
            free(b_free.at[1], right)

        for copy in c_copies(r):
            copy.start()

    def f4(r):
        b = lax.rem(r, DEEP)
        layer, s = 1 - lax.div(r, slots), lax.rem(r, slots)
        for copy in c_copies(r):
            copy.wait_recv()
        lanes = lax.broadcasted_iota(jnp.int32, (tall, 128), 1) // ROWS
        out = squares[...]
        for half, grad in ((0, gg), (1, gu)):
            for group in range(n // 4):
                cols = slice(half * wide + 128 * group, half * wide + 128 * (group + 1))
                total = fin[b, 0:tall, cols] + wholes[b, 0, 0:tall, cols].astype(F32) + wholes[b, 1, 0:tall, cols].astype(F32)
                total = total.astype(BF16).astype(F32)
                out = out + jnp.sum((total * total).reshape(tall // 8, 8, 128), axis=0)
                for place in range(4):
                    unit = slots * (4 * group + place) + s
                    where = pl.ds(pl.multiple_of(lax.div(unit, 4) * 128, 128), 128)
                    moved = pltpu.roll(total, lax.rem(lax.rem(unit, 4) + 4 - place, 4) * ROWS, 1)
                    grad[layer, :, where] = jnp.where(lanes == lax.rem(unit, 4), moved, grad[layer, :, where].astype(F32)).astype(BF16)
        for half in range(2):
            rows = slice(tall + ROWS * half, tall + ROWS * (half + 1))
            total = fin[b, rows, :] + wholes[b, 0, rows, :].astype(F32) + wholes[b, 1, rows, :].astype(F32)
            total = total.astype(BF16).astype(F32)
            gd[layer, pl.ds(pl.multiple_of(s * ROWS, ROWS), ROWS), 2 * wide * half : 2 * wide * (half + 1)] = total.astype(BF16)
            for lane in range(0, 2 * wide, 128):
                one = total[:, lane : lane + 128]
                out = out + jnp.sum((one * one).reshape(ROWS // 8, 8, 128), axis=0)
        squares[...] = out

        @pl.when(r + DEEP < chunks)
        def _():
            free(c_free.at[0], left)
            free(c_free.at[1], right)

    def turn(block, dst, start, size):
        for q in range(0, d, 256):
            dst[q : q + 256, pl.ds(start, size)] = block[:, q : q + 256].T.astype(BF16)

    def gates(rows, b):
        return gated(dot(va[rows, :], wgu_b[b].reshape(d, 2 * wide)))

    def gated(both):
        g, u = both[:, :wide], both[:, wide:]
        sig = jax.nn.sigmoid(g)
        silu = g * sig
        return silu, u * (sig + silu * (1.0 - sig)), (silu * u).astype(BF16)

    def gradients(r, a):
        p = lax.rem(r, 2)
        for m in range(2):
            g = dot(vat[512 * m : 512 * (m + 1), :], dgu[...]).astype(BF16)
            for i in range(512 // tall):
                j = m * (512 // tall) + i
                term[p, j % 2, j // 2, 0:tall, :] = g[tall * i : tall * (i + 1), :]
        hidden = act[a]
        for m in range(4):
            g = dot(vct[256 * m : 256 * (m + 1), :], hidden).T.astype(BF16)
            low = tall + ROWS * (m // 2)
            for j in range(n):
                term[p, j % 2, j // 2, low : low + ROWS, 256 * (m % 2) : 256 * (m % 2 + 1)] = g[ROWS * j : ROWS * (j + 1), :]

    def stashes(t, b):
        return [
            pltpu.make_async_copy(act.at[b], act_st.at[t], stash_sem.at[b, 0]),
            pltpu.make_async_copy(sgu.at[b], sgu_st.at[t], stash_sem.at[b, 1]),
        ]

    def saved(s):
        b = lax.rem(s, 2)
        return down_loads(s, b) + [
            pltpu.make_async_copy(act_st.at[s], act.at[b], saved_sem.at[b, 0]),
            pltpu.make_async_copy(sgu_st.at[s], sgu.at[b], saved_sem.at[b, 1]),
        ]

    x_in = pltpu.make_async_copy(x, va, in_sem.at[0])
    dy_in = pltpu.make_async_copy(dy, vc, in_sem.at[1])
    x_in.start()
    dy_in.start()
    barrier = pltpu.get_barrier_semaphore()
    for i in range(1, n):
        pl.semaphore_signal(barrier, inc=1, device_id={"dp": lax.rem(me + i, n)}, device_id_type=MESH)
    prepare(0)
    pl.semaphore_wait(barrier, n - 1)
    e1(0)
    e1(1)
    x_in.wait()

    def first(i, _):
        start = pl.multiple_of(i * 256, 256)
        rows = pl.ds(start, 256)
        h = va[rows, :].astype(F32)
        a = (h * lax.rsqrt(jnp.mean(h * h, -1, keepdims=True) + 1e-6)).astype(BF16)
        va[rows, :] = a
        turn(a.astype(F32), vat, start, 256)
        acc[rows, :] = jnp.zeros((256, d), F32)
        return 0

    lax.fori_loop(0, tokens // 256, first, 0)
    a0t_out = pltpu.make_async_copy(vat, a0t_st, in_sem.at[2])
    a0t_out.start()
    e2(0)
    e1(2)
    dy_in.wait()

    def second(i, _):
        start = pl.multiple_of(i * 256, 256)
        turn(vc[pl.ds(start, 256), :].astype(F32), vct, start, 256)
        return 0

    lax.fori_loop(0, tokens // 256, second, 0)
    e3(0)
    e2(1)
    e1(3)
    e4(0)
    gg[...] = jnp.zeros_like(gg)
    gu[...] = jnp.zeros_like(gu)
    squares[...] = jnp.zeros_like(squares)

    def forward(t, _):
        e2(t + 2)
        e3(t + 1)
        e1(t + 4)
        for copy in loads(t):
            copy.wait()
        b = lax.rem(t, 2)

        @pl.when(t >= 2)
        def _():
            for copy in stashes(t - 2, b):
                copy.wait()

        def work(i, _):
            rows = pl.ds(pl.multiple_of(i * BLOCK, BLOCK), BLOCK)
            silu, slope, hidden = gates(rows, b)
            act[b, rows, :] = hidden
            sgu[b, rows, 0:wide] = slope
            sgu[b, rows, wide:] = silu
            acc[rows, :] += dot(hidden, wd_b[b].reshape(n * ROWS, d))
            return 0

        lax.fori_loop(0, blocks // 2, work, 0)
        e4(t + 1)
        lax.fori_loop(blocks // 2, blocks, work, 0)
        for copy in stashes(t, b):
            copy.start()
        return 0

    lax.fori_loop(0, slots, forward, 0)
    x_in.start()
    a0t_out.wait()
    for t in (slots - 2, slots - 1):
        for copy in stashes(t, t % 2):
            copy.wait()
    x_in.wait()

    def between(i, _):
        start = pl.multiple_of(i * 256, 256)
        rows = pl.ds(start, 256)
        h = (va[rows, :].astype(F32) + acc[rows, :].astype(BF16).astype(F32)).astype(BF16).astype(F32)
        sgu[0, rows, :] = h[:, : 2 * wide]
        sgu[1, rows, :] = h[:, 2 * wide :]
        a = (h * lax.rsqrt(jnp.mean(h * h, -1, keepdims=True) + 1e-6)).astype(BF16)
        va[rows, :] = a
        turn(a.astype(F32), vat, start, 256)
        acc[rows, :] = jnp.zeros((256, d), F32)
        return 0

    lax.fori_loop(0, tokens // 256, between, 0)

    def both_ways(t, _):
        r = t - slots

        @pl.when(t + 2 < chunks)
        def _():
            e2(t + 2)

        @pl.when(t + 4 < chunks)
        def _():
            e1(t + 4)

        for copy in loads(t):
            copy.wait()
        b = lax.rem(t, 2)

        def ahead(i):
            rows = slice(i * BLOCK, (i + 1) * BLOCK)
            both = dot(va[rows, :], wgu_b[b].reshape(d, 2 * wide))
            return both, dot_t(vc[rows, :], wd_b[b].reshape(n * ROWS, d))

        def behind(i, both, by):
            rows = slice(i * BLOCK, (i + 1) * BLOCK)
            silu, slope, hidden = gated(both)
            by = by.astype(BF16).astype(F32)
            act[0, rows, :] = hidden
            dgu[rows, 0:wide] = (by * slope).astype(BF16)
            dgu[rows, wide:] = (by * silu).astype(BF16)
            acc[rows, :] += dot_t(dgu[rows, :], wgu_b[b].reshape(d, 2 * wide))

        def work(start, stop):
            held = ahead(start)
            for i in range(start, stop):
                later = ahead(i + 1) if i + 1 < stop else None
                behind(i, *held)
                held = later

        work(0, blocks // 2)

        @pl.when(r >= 4)
        def _():
            f4(r - 4)

        @pl.when(r >= 1)
        def _():
            f2(r - 1)

        @pl.when(t + 1 < chunks)
        def _():
            e3(t + 1)

        work(blocks // 2, blocks)

        @pl.when(t + 1 < chunks)
        def _():
            e4(t + 1)

        @pl.when(r >= 2)
        def _():
            f3(r - 2)

        gradients(r, 0)
        f1(r)
        return 0

    lax.fori_loop(slots, chunks, both_ways, 0)
    a0t_in = pltpu.make_async_copy(a0t_st, vat, in_sem.at[2])
    a0t_in.start()
    for copy in saved(0)[:3]:
        copy.start()

    def back(i, _):
        start = pl.multiple_of(i * 256, 256)
        rows = pl.ds(start, 256)
        h = jnp.concatenate([sgu[0, rows, :], sgu[1, rows, :]], axis=1)
        da = acc[rows, :].astype(BF16).astype(F32)
        scale = lax.rsqrt(jnp.mean(h * h, -1, keepdims=True) + 1e-6)
        along = jnp.mean(da * h, -1, keepdims=True)
        by_h = (da * scale - h * (scale * scale * scale * along)).astype(BF16).astype(F32)
        by_h = (vc[rows, :].astype(F32) + by_h).astype(BF16)
        vc[rows, :] = by_h
        turn(by_h.astype(F32), vct, start, 256)
        return 0

    lax.fori_loop(0, tokens // 256, back, 0)
    saved(0)[3].start()
    a0t_in.wait()

    def backward(t, _):
        r, s = t - slots, t - chunks
        b = lax.rem(s, 2)
        for copy in saved(s):
            copy.wait()

        @pl.when(s + 1 < slots)
        def _():
            for copy in saved(s + 1):
                copy.start()

        def ahead(i):
            return dot_t(vc[i * BLOCK : (i + 1) * BLOCK, :], wd_b[b].reshape(n * ROWS, d))

        held = ahead(0)
        for i in range(blocks):
            later = ahead(i + 1) if i + 1 < blocks else None
            rows = slice(i * BLOCK, (i + 1) * BLOCK)
            by = held.astype(BF16).astype(F32)
            dgu[rows, 0:wide] = (by * sgu[b, rows, 0:wide]).astype(BF16)
            dgu[rows, wide:] = (by * sgu[b, rows, wide:]).astype(BF16)
            held = later

        f4(r - 4)
        f2(r - 1)
        f3(r - 2)
        gradients(r, b)
        f1(r)
        return 0

    lax.fori_loop(chunks, chunks + slots, backward, 0)

    f4(chunks - 4)
    f2(chunks - 1)
    f3(chunks - 2)
    f4(chunks - 3)
    f3(chunks - 1)
    f4(chunks - 2)
    f4(chunks - 1)
    for k in range(chunks - OWN, chunks):
        for copy in own_copies(k) + forwards(k) + [last_forward(k)]:
            copy.wait_send()
    for r in range(chunks - DEEP, chunks):
        for copy in b_copies(r) + c_copies(r):
            copy.wait_send()

    norms[me] = squares[...]
    sends = [
        remote(squares, norms.at[me], norm_send.at[i], norm_recv.at[i], lax.rem(me + i + 1, n)) for i in range(n - 1)
    ]
    for copy in sends:
        copy.start()
    for i in range(n - 1):
        source = lax.rem(me + n - i - 1, n)
        remote(norms.at[source], norms.at[source], norm_send.at[i], norm_recv.at[i], me).wait_recv()
    for copy in sends:
        copy.wait_send()
    total = jnp.sum(norms[...])
    fac[...] = jnp.minimum(1.0, 0.5 * lax.rsqrt(jnp.full((8, 128), total / count, F32) + 1e-30))[0:1, 0:1]


def gradients_of(n, x, dy, wg, wu, wd):
    layers, tall, ff = wg.shape
    down, d = wd.shape[1:]
    tokens = x.shape[0]
    slots, wide = down // ROWS, n * ROWS
    chunks, high = layers * slots, tall + 2 * ROWS
    chips = n // 2
    assert layers == 2 and chips == 4 and d == 4 * wide and tokens % BLOCK == 0 and down % ROWS == 0
    hbm, vmem = pl.BlockSpec(memory_space=pl.ANY), pl.BlockSpec(memory_space=pltpu.VMEM)
    dma, plain = pltpu.SemaphoreType.DMA, pltpu.SemaphoreType.REGULAR
    out = pl.pallas_call(
        functools.partial(kernel, n, float(n * (wg.size + wu.size + wd.size))),
        out_shape=(
            jax.ShapeDtypeStruct((chunks, n, high, 2 * wide), BF16),
            jax.ShapeDtypeStruct((slots, tokens, wide), BF16),
            jax.ShapeDtypeStruct((slots, tokens, 2 * wide), F32),
            jax.ShapeDtypeStruct((d, tokens), BF16),
            jax.ShapeDtypeStruct(wg.shape, BF16),
            jax.ShapeDtypeStruct(wu.shape, BF16),
            jax.ShapeDtypeStruct(wd.shape, BF16),
            jax.ShapeDtypeStruct((1, 1), F32),
        ),
        in_specs=[hbm, hbm, vmem, vmem, vmem],
        out_specs=(hbm, hbm, hbm, hbm, vmem, vmem, vmem, vmem),
        scratch_shapes=[
            pltpu.VMEM((tokens, d), BF16),
            pltpu.VMEM((d, tokens), BF16),
            pltpu.VMEM((tokens, d), BF16),
            pltpu.VMEM((d, tokens), BF16),
            pltpu.VMEM((tokens, d), F32),
            pltpu.VMEM((2, tokens, wide), BF16),
            pltpu.VMEM((2, tokens, 2 * wide), F32),
            pltpu.VMEM((tokens, 2 * wide), BF16),
            pltpu.VMEM((2, n, tall, 2 * wide), BF16),
            pltpu.VMEM((2, n, ROWS, d), BF16),
            pltpu.VMEM((OWN, high, 2 * wide), BF16),
            pltpu.VMEM((2, 2, chips, high, 2 * wide), BF16),
            pltpu.VMEM((2, chips, high, 2 * wide), BF16),
            pltpu.VMEM((DEEP, 3, high, 2 * wide), BF16),
            pltpu.VMEM((DEEP, high, 2 * wide), F32),
            pltpu.VMEM((DEEP, 2, high // 2, 2 * wide), BF16),
            pltpu.VMEM((DEEP, 2, high, 2 * wide), BF16),
            pltpu.VMEM((8, 128), F32),
            pltpu.VMEM((n, 8, 128), F32),
            dma((3,)),
            dma((OWN, 3)),
            dma((OWN,)),
            dma((OWN, 2)),
            dma((OWN, 2)),
            dma((OWN, 4)),
            dma((OWN, 5)),
            dma((2, 3)),
            dma((2, 2)),
            dma((2, 2)),
            dma((2,)),
            dma((2,)),
            dma((DEEP, 2)),
            dma((DEEP, 2)),
            dma((DEEP, 2)),
            dma((DEEP, 2)),
            dma((n - 1,)),
            dma((n - 1,)),
            plain,
            plain((2,)),
            plain((2,)),
        ],
        compiler_params=pltpu.CompilerParams(collective_id=0, has_side_effects=True, vmem_limit_bytes=67043328),
        cost_estimate=pl.CostEstimate(
            flops=30 * tokens * d * ff, bytes_accessed=200_000_000, transcendentals=2 * layers * tokens * ff
        ),
    )(x, dy, wg, wu, wd)
    return out[4:7], out[7].reshape(())


def adamw(w, m, v, g):
    m = 0.9 * m + 0.1 * g
    v = 0.95 * v + 0.05 * g * g
    step = m * lax.rsqrt(v + 1e-8) + 0.1 * w
    return (w - 0.02 * step).astype(BF16), m, v


def solution(mesh):
    n = mesh.shape["dp"]

    def step(x, dy, *arrays):
        weights, m, v = (arrays[i : i + 3] for i in (0, 3, 6))
        gradients, factor = gradients_of(n, x[0], dy[0], *weights)
        new = [
            adamw(w.astype(F32), m, v, g.astype(F32) * factor) for w, m, v, g in zip(weights, m, v, gradients, strict=True)
        ]
        return tuple(one[which] for which in range(3) for one in new)

    states, cut = P(("rep", "dp"), None, None), P(None, "dp", None)
    return jax.shard_map(
        step,
        mesh=mesh,
        in_specs=(states, states) + (cut,) * 9,
        out_specs=(P("rep", "dp", None),) * 9,
        check_vma=False,
    )
```

```python
import functools

import jax
import jax.numpy as jnp
from jax import lax
from jax.experimental import pallas as pl
from jax.experimental.pallas import tpu as pltpu
from jax.sharding import PartitionSpec as P

MESH = pl.DeviceIdType.MESH
F32, BF16 = jnp.float32, jnp.bfloat16
ROWS = 32
BLOCK = 512
OWN, DEEP = 6, 3


def dot(a, b):
    return lax.dot_general(a, b, (((1,), (0,)), ((), ())), preferred_element_type=F32)


def dot_t(a, b):
    return lax.dot_general(a, b, (((1,), (1,)), ((), ())), preferred_element_type=F32)


def kernel(
    n, count,
    x, dy, wg, wu, wd,
    gath, act_st, sgu_st, a0t_st, gg, gu, gd, fac,
    va, vat, vc, vct, acc, act, sgu, dgu, rest, wgu_b, wd_b,
    own, term, pair, part, fin, halves, wholes, squares, norms,
    in_sem, own_send, own_local, full_recv, half_recv, part_recv, fwd_send, load_sem, stash_sem, saved_sem,
    pair_send, pair_recv, b_send, b_recv, c_send, c_recv, norm_send, norm_recv,
    pair_free, b_free, c_free,
):
    me = lax.axis_index("dp")
    chips = n // 2
    c, at = lax.rem(me, 2), lax.div(me, 2)
    over = lax.rem(at + 2, chips)
    right_chip, left_chip = lax.rem(at + 1, chips), lax.rem(at + chips - 1, chips)
    partner = at * 2 + 1 - c
    right, left, far = right_chip * 2 + c, left_chip * 2 + c, over * 2 + c
    tokens, d = va.shape
    wide = wgu_b.shape[3] // 2
    slots = wd.shape[1] // ROWS
    layers = wd.shape[0]
    chunks = layers * slots
    blocks = tokens // BLOCK
    high = own.shape[1]
    mid = high // 2
    tall = wg.shape[1]

    def remote(src, dst, send, recv, to):
        return pltpu.make_async_remote_copy(
            src_ref=src, dst_ref=dst, send_sem=send, recv_sem=recv, device_id={"dp": to}, device_id_type=MESH
        )

    def prepare(k):
        b, layer, s = lax.rem(k, OWN), lax.div(k, slots), lax.rem(k, slots)
        lanes = lax.broadcasted_iota(jnp.int32, (tall, 128), 1) // ROWS
        for w, base in ((wg, 0), (wu, wide)):
            for group in range(n // 4):
                total = None
                for place in range(4):
                    unit = slots * (4 * group + place) + s
                    piece = w[layer, :, pl.ds(pl.multiple_of(lax.div(unit, 4) * 128, 128), 128)].astype(F32)
                    piece = pltpu.roll(piece, lax.rem(place + 4 - lax.rem(unit, 4), 4) * ROWS, 1)
                    total = piece if total is None else jnp.where(lanes == place, piece, total)
                own[b, 0:tall, base + 128 * group : base + 128 * (group + 1)] = total.astype(BF16)
        rows = wd[layer, pl.ds(pl.multiple_of(s * ROWS, ROWS), ROWS), :]
        own[b, tall : tall + ROWS, :] = rows[:, : 2 * wide]
        own[b, tall + ROWS : high, :] = rows[:, 2 * wide :]

    def own_copies(k):
        b = lax.rem(k, OWN)
        return [
            remote(own.at[b], gath.at[k, me], own_send.at[b, 0], full_recv.at[b, 0], right),
            remote(own.at[b], gath.at[k, me], own_send.at[b, 1], full_recv.at[b, 1], left),
            remote(own.at[b], gath.at[k, me], own_send.at[b, 2], part_recv.at[b, 0], partner),
        ]

    def own_here(k):
        b = lax.rem(k, OWN)
        return pltpu.make_async_copy(own.at[b], gath.at[k, me], own_local.at[b])

    def e1(k):
        for copy in own_copies(k):
            copy.start()
        own_here(k).start()

        @pl.when(k + 1 < chunks)
        def _():
            @pl.when(k + 1 >= OWN)
            def _():
                for copy in own_copies(k + 1 - OWN):
                    copy.wait_send()

            prepare(k + 1)

    def arrived(region, recv):
        remote(region, region, fwd_send.at[0, 0], recv, me).wait_recv()

    def forwards(k):
        b = lax.rem(k, OWN)
        return [
            remote(gath.at[k, left, 0:mid], gath.at[k, left, 0:mid], fwd_send.at[b, 0], half_recv.at[b, 0], right),
            remote(gath.at[k, right, mid:high], gath.at[k, right, mid:high], fwd_send.at[b, 1], half_recv.at[b, 1], left),
            remote(gath.at[k, left], gath.at[k, left], fwd_send.at[b, 2], part_recv.at[b, 1], partner),
            remote(gath.at[k, right], gath.at[k, right], fwd_send.at[b, 3], part_recv.at[b, 2], partner),
        ]

    def last_forward(k):
        b = lax.rem(k, OWN)
        return remote(gath.at[k, far], gath.at[k, far], fwd_send.at[b, 4], part_recv.at[b, 3], partner)

    def e2(k):
        b = lax.rem(k, OWN)

        @pl.when(k >= OWN)
        def _():
            for copy in forwards(k - OWN):
                copy.wait_send()

        arrived(gath.at[k, left], full_recv.at[b, 0])
        arrived(gath.at[k, right], full_recv.at[b, 1])
        for copy in forwards(k):
            copy.start()

    def e3(k):
        b = lax.rem(k, OWN)

        @pl.when(k >= OWN)
        def _():
            last_forward(k - OWN).wait_send()

        arrived(gath.at[k, far, 0:mid], half_recv.at[b, 0])
        arrived(gath.at[k, far, mid:high], half_recv.at[b, 1])
        last_forward(k).start()

    def down_loads(k, b):
        return [
            pltpu.make_async_copy(gath.at[k, :, tall : tall + ROWS], wd_b.at[b, :, :, 0 : 2 * wide], load_sem.at[b, 0]),
            pltpu.make_async_copy(gath.at[k, :, tall + ROWS : high], wd_b.at[b, :, :, 2 * wide : 4 * wide], load_sem.at[b, 1]),
        ]

    def loads(k):
        b = lax.rem(k, 2)
        return [pltpu.make_async_copy(gath.at[k, :, 0:tall], wgu_b.at[b], load_sem.at[b, 2])] + down_loads(k, b)

    def e4(k):
        b = lax.rem(k, OWN)
        other = 1 - 2 * c
        own_here(k).wait()
        for i, j in enumerate((me, left, right, far)):
            arrived(gath.at[k, j + other], part_recv.at[b, i])
        for copy in loads(k):
            copy.start()

    def pair_copy(r):
        b = lax.rem(r, 2)
        return remote(term.at[b, 1 - c], pair.at[b], pair_send.at[b], pair_recv.at[b], partner)

    def b_copies(r):
        b = lax.rem(r, DEEP)
        return [
            remote(part.at[b, 1, 0:mid], halves.at[b, 0], b_send.at[b, 0], b_recv.at[b, 0], right),
            remote(part.at[b, 1, mid:high], halves.at[b, 1], b_send.at[b, 1], b_recv.at[b, 1], left),
        ]

    def c_copies(r):
        b = lax.rem(r, DEEP)
        return [
            remote(part.at[b, 0], wholes.at[b, 0], c_send.at[b, 0], c_recv.at[b, 0], right),
            remote(part.at[b, 2], wholes.at[b, 1], c_send.at[b, 1], c_recv.at[b, 1], left),
        ]

    def free(sem, to):
        pl.semaphore_signal(sem, inc=1, device_id={"dp": to}, device_id_type=MESH)

    STRIP = 48

    def f1(r):
        @pl.when(r >= 2)
        def _():
            pl.semaphore_wait(pair_free, 1)

        pair_copy(r).start()

    def f2(r):
        b, p = lax.rem(r, DEEP), lax.rem(r, 2)

        @pl.when(r >= DEEP)
        def _():
            for copy in b_copies(r - DEEP) + c_copies(r - DEEP):
                copy.wait_send()
            pl.semaphore_wait(b_free.at[0], 1)
            pl.semaphore_wait(b_free.at[1], 1)

        pair_copy(r).wait_recv()
        for away, chip in ((2, over), (1, right_chip), (3, left_chip), (0, at)):
            for row in range(0, high, STRIP):
                total = term[p, c, chip, row : row + STRIP, :].astype(F32) + pair[p, chip, row : row + STRIP, :].astype(F32)
                if away:
                    part[b, away - 1, row : row + STRIP, :] = total.astype(BF16)
                else:
                    fin[b, row : row + STRIP, :] = total
        for copy in b_copies(r):
            copy.start()
        pair_copy(r).wait_send()

        @pl.when(r + 2 < chunks)
        def _():
            free(pair_free, partner)

    def f3(r):
        b = lax.rem(r, DEEP)

        @pl.when(r >= DEEP)
        def _():
            pl.semaphore_wait(c_free.at[0], 1)
            pl.semaphore_wait(c_free.at[1], 1)

        for i in range(2):
            b_copies(r)[i].wait_recv()
            start = mid * i
            for row in range(0, mid, STRIP):
                total = part[b, 2 * i, start + row : start + row + STRIP, :].astype(F32) + halves[b, i, row : row + STRIP, :].astype(F32)
                part[b, 2 * i, start + row : start + row + STRIP, :] = total.astype(BF16)

        @pl.when(r + DEEP < chunks)
        def _():
            free(b_free.at[0], left)
            free(b_free.at[1], right)

        for copy in c_copies(r):
            copy.start()

    def f4(r):
        b = lax.rem(r, DEEP)
        layer, s = 1 - lax.div(r, slots), lax.rem(r, slots)
        for copy in c_copies(r):
            copy.wait_recv()
        lanes = lax.broadcasted_iota(jnp.int32, (tall, 128), 1) // ROWS
        out = squares[...]
        for half, grad in ((0, gg), (1, gu)):
            for group in range(n // 4):
                cols = slice(half * wide + 128 * group, half * wide + 128 * (group + 1))
                total = fin[b, 0:tall, cols] + wholes[b, 0, 0:tall, cols].astype(F32) + wholes[b, 1, 0:tall, cols].astype(F32)
                total = total.astype(BF16).astype(F32)
                out = out + jnp.sum((total * total).reshape(tall // 8, 8, 128), axis=0)
                for place in range(4):
                    unit = slots * (4 * group + place) + s
                    where = pl.ds(pl.multiple_of(lax.div(unit, 4) * 128, 128), 128)
                    moved = pltpu.roll(total, lax.rem(lax.rem(unit, 4) + 4 - place, 4) * ROWS, 1)
                    grad[layer, :, where] = jnp.where(lanes == lax.rem(unit, 4), moved, grad[layer, :, where].astype(F32)).astype(BF16)
        for half in range(2):
            rows = slice(tall + ROWS * half, tall + ROWS * (half + 1))
            total = fin[b, rows, :] + wholes[b, 0, rows, :].astype(F32) + wholes[b, 1, rows, :].astype(F32)
            total = total.astype(BF16).astype(F32)
            gd[layer, pl.ds(pl.multiple_of(s * ROWS, ROWS), ROWS), 2 * wide * half : 2 * wide * (half + 1)] = total.astype(BF16)
            for lane in range(0, 2 * wide, 128):
                one = total[:, lane : lane + 128]
                out = out + jnp.sum((one * one).reshape(ROWS // 8, 8, 128), axis=0)
        squares[...] = out

        @pl.when(r + DEEP < chunks)
        def _():
            free(c_free.at[0], left)
            free(c_free.at[1], right)

    def turn(block, dst, start, size):
        for q in range(0, d, 256):
            dst[q : q + 256, pl.ds(start, size)] = block[:, q : q + 256].T

    def gates(rows, b):
        return gated(dot(va[rows, :], wgu_b[b].reshape(d, 2 * wide)))

    def gated(both):
        g, u = both[:, :wide], both[:, wide:]
        sig = jax.nn.sigmoid(g)
        silu = g * sig
        return silu, u * (sig + silu * (1.0 - sig)), (silu * u).astype(BF16)

    def gradients(r, a):
        p = lax.rem(r, 2)
        for m in range(2):
            g = dot(vat[512 * m : 512 * (m + 1), :], dgu[...]).astype(BF16)
            for i in range(512 // tall):
                j = m * (512 // tall) + i
                term[p, j % 2, j // 2, 0:tall, :] = g[tall * i : tall * (i + 1), :]
        hidden = act[a]
        for m in range(4):
            g = dot(vct[256 * m : 256 * (m + 1), :], hidden).T.astype(BF16)
            low = tall + ROWS * (m // 2)
            for j in range(n):
                term[p, j % 2, j // 2, low : low + ROWS, 256 * (m % 2) : 256 * (m % 2 + 1)] = g[ROWS * j : ROWS * (j + 1), :]

    def stashes(t, b):
        return [
            pltpu.make_async_copy(act.at[b], act_st.at[t], stash_sem.at[b, 0]),
            pltpu.make_async_copy(sgu.at[b], sgu_st.at[t], stash_sem.at[b, 1]),
        ]

    def saved(s):
        b = lax.rem(s, 2)
        return down_loads(s, b) + [
            pltpu.make_async_copy(act_st.at[s], act.at[b], saved_sem.at[b, 0]),
            pltpu.make_async_copy(sgu_st.at[s], sgu.at[b], saved_sem.at[b, 1]),
        ]

    x_in = pltpu.make_async_copy(x, va, in_sem.at[0])
    dy_in = pltpu.make_async_copy(dy, vc, in_sem.at[1])
    x_in.start()
    dy_in.start()
    barrier = pltpu.get_barrier_semaphore()
    for i in range(1, n):
        pl.semaphore_signal(barrier, inc=1, device_id={"dp": lax.rem(me + i, n)}, device_id_type=MESH)
    prepare(0)
    pl.semaphore_wait(barrier, n - 1)
    e1(0)
    e1(1)
    x_in.wait()

    def first(i, _):
        start = pl.multiple_of(i * 256, 256)
        rows = pl.ds(start, 256)
        h = va[rows, :].astype(F32)
        a = (h * lax.rsqrt(jnp.mean(h * h, -1, keepdims=True) + 1e-6)).astype(BF16)
        va[rows, :] = a
        turn(a, vat, start, 256)
        acc[rows, :] = jnp.zeros((256, d), F32)
        return 0

    lax.fori_loop(0, tokens // 256, first, 0)
    a0t_out = pltpu.make_async_copy(vat, a0t_st, in_sem.at[2])
    a0t_out.start()
    e2(0)
    e1(2)
    dy_in.wait()

    def second(i, _):
        start = pl.multiple_of(i * 256, 256)
        turn(vc[pl.ds(start, 256), :], vct, start, 256)
        return 0

    lax.fori_loop(0, tokens // 256, second, 0)
    e3(0)
    e2(1)
    e1(3)
    e4(0)
    gg[...] = jnp.zeros_like(gg)
    gu[...] = jnp.zeros_like(gu)
    squares[...] = jnp.zeros_like(squares)

    half = tokens // 2
    x_again = [
        pltpu.make_async_copy(x.at[i * half : (i + 1) * half], va.at[i * half : (i + 1) * half], in_sem.at[i]) for i in range(2)
    ]

    def forward(t, _):
        e2(t + 2)
        e3(t + 1)
        e1(t + 4)
        for copy in loads(t):
            copy.wait()
        b = lax.rem(t, 2)

        @pl.when(t >= 2)
        def _():
            for copy in stashes(t - 2, b):
                copy.wait()

        def work(i, _):
            rows = pl.ds(pl.multiple_of(i * BLOCK, BLOCK), BLOCK)
            silu, slope, hidden = gates(rows, b)
            act[b, rows, :] = hidden
            sgu[b, rows, 0:wide] = slope
            sgu[b, rows, wide:] = silu
            acc[rows, :] += dot(hidden, wd_b[b].reshape(n * ROWS, d))
            return 0

        lax.fori_loop(0, blocks // 2, work, 0)
        e4(t + 1)

        @pl.when(t == slots - 1)
        def _():
            x_again[0].start()

        lax.fori_loop(blocks // 2, blocks, work, 0)
        for copy in stashes(t, b):
            copy.start()
        return 0

    lax.fori_loop(0, slots, forward, 0)
    x_again[1].start()
    a0t_out.wait()
    last = (slots - 1) % 2
    for copy in stashes(slots - 2, 1 - last):
        copy.wait()
    x_again[0].wait()

    def between(i, _):
        start = pl.multiple_of(i * 256, 256)
        rows = pl.ds(start, 256)
        h = (va[rows, :].astype(F32) + acc[rows, :].astype(BF16).astype(F32)).astype(BF16).astype(F32)
        sgu[1 - last, rows, :] = h[:, : 2 * wide]
        act[1 - last, rows, :] = h[:, 2 * wide : 3 * wide].astype(BF16)
        rest[rows, :] = h[:, 3 * wide :].astype(BF16)
        a = (h * lax.rsqrt(jnp.mean(h * h, -1, keepdims=True) + 1e-6)).astype(BF16)
        va[rows, :] = a
        turn(a, vat, start, 256)
        acc[rows, :] = jnp.zeros((256, d), F32)
        return 0

    lax.fori_loop(0, half // 256, between, 0)
    x_again[1].wait()
    lax.fori_loop(half // 256, tokens // 256, between, 0)
    for copy in stashes(slots - 1, last):
        copy.wait()

    def both_ways(t, _):
        r = t - slots

        @pl.when(t + 2 < chunks)
        def _():
            e2(t + 2)

        @pl.when(t + 4 < chunks)
        def _():
            e1(t + 4)

        for copy in loads(t):
            copy.wait()
        b = lax.rem(t, 2)

        def ahead(i):
            rows = slice(i * BLOCK, (i + 1) * BLOCK)
            both = dot(va[rows, :], wgu_b[b].reshape(d, 2 * wide))
            return both, dot_t(vc[rows, :], wd_b[b].reshape(n * ROWS, d))

        def behind(i, both, by):
            rows = slice(i * BLOCK, (i + 1) * BLOCK)
            silu, slope, hidden = gated(both)
            by = by.astype(BF16).astype(F32)
            act[last, rows, :] = hidden
            dgu[rows, 0:wide] = (by * slope).astype(BF16)
            dgu[rows, wide:] = (by * silu).astype(BF16)
            acc[rows, :] += dot_t(dgu[rows, :], wgu_b[b].reshape(d, 2 * wide))

        def work(start, stop):
            held = ahead(start)
            for i in range(start, stop):
                later = ahead(i + 1) if i + 1 < stop else None
                behind(i, *held)
                held = later

        work(0, blocks // 2)

        @pl.when(r >= 4)
        def _():
            f4(r - 4)

        @pl.when(r >= 1)
        def _():
            f2(r - 1)

        @pl.when(t + 1 < chunks)
        def _():
            e3(t + 1)

        work(blocks // 2, blocks)

        @pl.when(t + 1 < chunks)
        def _():
            e4(t + 1)

        @pl.when(r >= 2)
        def _():
            f3(r - 2)

        gradients(r, last)
        f1(r)
        return 0

    lax.fori_loop(slots, chunks, both_ways, 0)
    a0t_in = pltpu.make_async_copy(a0t_st, vat, in_sem.at[2])
    a0t_in.start()
    for copy in saved(0):
        copy.start()

    def back(i, _):
        start = pl.multiple_of(i * 256, 256)
        rows = pl.ds(start, 256)
        h = jnp.concatenate([sgu[1 - last, rows, :], act[1 - last, rows, :].astype(F32), rest[rows, :].astype(F32)], axis=1)
        da = acc[rows, :].astype(BF16).astype(F32)
        scale = lax.rsqrt(jnp.mean(h * h, -1, keepdims=True) + 1e-6)
        along = jnp.mean(da * h, -1, keepdims=True)
        by_h = (da * scale - h * (scale * scale * scale * along)).astype(BF16).astype(F32)
        by_h = (vc[rows, :].astype(F32) + by_h).astype(BF16)
        vc[rows, :] = by_h
        turn(by_h, vct, start, 256)
        return 0

    lax.fori_loop(0, tokens // 256, back, 0)
    a0t_in.wait()

    def backward(t, _):
        r, s = t - slots, t - chunks
        b = lax.rem(s, 2)
        for copy in saved(s):
            copy.wait()

        @pl.when(s + 1 < slots)
        def _():
            for copy in saved(s + 1):
                copy.start()

        def ahead(i):
            return dot_t(vc[i * BLOCK : (i + 1) * BLOCK, :], wd_b[b].reshape(n * ROWS, d))

        held = ahead(0)
        for i in range(blocks):
            later = ahead(i + 1) if i + 1 < blocks else None
            rows = slice(i * BLOCK, (i + 1) * BLOCK)
            by = held.astype(BF16).astype(F32)
            dgu[rows, 0:wide] = (by * sgu[b, rows, 0:wide]).astype(BF16)
            dgu[rows, wide:] = (by * sgu[b, rows, wide:]).astype(BF16)
            held = later

        f4(r - 4)
        f2(r - 1)
        f3(r - 2)
        gradients(r, b)
        f1(r)
        return 0

    lax.fori_loop(chunks, chunks + slots, backward, 0)

    f4(chunks - 4)
    f2(chunks - 1)
    f3(chunks - 2)
    f4(chunks - 3)
    f3(chunks - 1)
    f4(chunks - 2)
    f4(chunks - 1)
    for k in range(chunks - OWN, chunks):
        for copy in own_copies(k) + forwards(k) + [last_forward(k)]:
            copy.wait_send()
    for r in range(chunks - DEEP, chunks):
        for copy in b_copies(r) + c_copies(r):
            copy.wait_send()

    norms[me] = squares[...]
    sends = [
        remote(squares, norms.at[me], norm_send.at[i], norm_recv.at[i], lax.rem(me + i + 1, n)) for i in range(n - 1)
    ]
    for copy in sends:
        copy.start()
    for i in range(n - 1):
        source = lax.rem(me + n - i - 1, n)
        remote(norms.at[source], norms.at[source], norm_send.at[i], norm_recv.at[i], me).wait_recv()
    for copy in sends:
        copy.wait_send()
    total = jnp.sum(norms[...])
    fac[...] = jnp.minimum(1.0, 0.5 * lax.rsqrt(jnp.full((8, 128), total / count, F32) + 1e-30))[0:1, 0:1]


def gradients_of(n, x, dy, wg, wu, wd):
    layers, tall, ff = wg.shape
    down, d = wd.shape[1:]
    tokens = x.shape[0]
    slots, wide = down // ROWS, n * ROWS
    chunks, high = layers * slots, tall + 2 * ROWS
    chips = n // 2
    assert layers == 2 and chips == 4 and d == 4 * wide and tokens % BLOCK == 0 and down % ROWS == 0
    hbm, vmem = pl.BlockSpec(memory_space=pl.ANY), pl.BlockSpec(memory_space=pltpu.VMEM)
    dma, plain = pltpu.SemaphoreType.DMA, pltpu.SemaphoreType.REGULAR
    out = pl.pallas_call(
        functools.partial(kernel, n, float(n * (wg.size + wu.size + wd.size))),
        out_shape=(
            jax.ShapeDtypeStruct((chunks, n, high, 2 * wide), BF16),
            jax.ShapeDtypeStruct((slots, tokens, wide), BF16),
            jax.ShapeDtypeStruct((slots, tokens, 2 * wide), F32),
            jax.ShapeDtypeStruct((d, tokens), BF16),
            jax.ShapeDtypeStruct(wg.shape, BF16),
            jax.ShapeDtypeStruct(wu.shape, BF16),
            jax.ShapeDtypeStruct(wd.shape, BF16),
            jax.ShapeDtypeStruct((1, 1), F32),
        ),
        in_specs=[hbm, hbm, vmem, vmem, vmem],
        out_specs=(hbm, hbm, hbm, hbm, vmem, vmem, vmem, vmem),
        scratch_shapes=[
            pltpu.VMEM((tokens, d), BF16),
            pltpu.VMEM((d, tokens), BF16),
            pltpu.VMEM((tokens, d), BF16),
            pltpu.VMEM((d, tokens), BF16),
            pltpu.VMEM((tokens, d), F32),
            pltpu.VMEM((2, tokens, wide), BF16),
            pltpu.VMEM((2, tokens, 2 * wide), F32),
            pltpu.VMEM((tokens, 2 * wide), BF16),
            pltpu.VMEM((tokens, wide), BF16),
            pltpu.VMEM((2, n, tall, 2 * wide), BF16),
            pltpu.VMEM((2, n, ROWS, d), BF16),
            pltpu.VMEM((OWN, high, 2 * wide), BF16),
            pltpu.VMEM((2, 2, chips, high, 2 * wide), BF16),
            pltpu.VMEM((2, chips, high, 2 * wide), BF16),
            pltpu.VMEM((DEEP, 3, high, 2 * wide), BF16),
            pltpu.VMEM((DEEP, high, 2 * wide), F32),
            pltpu.VMEM((DEEP, 2, high // 2, 2 * wide), BF16),
            pltpu.VMEM((DEEP, 2, high, 2 * wide), BF16),
            pltpu.VMEM((8, 128), F32),
            pltpu.VMEM((n, 8, 128), F32),
            dma((3,)),
            dma((OWN, 3)),
            dma((OWN,)),
            dma((OWN, 2)),
            dma((OWN, 2)),
            dma((OWN, 4)),
            dma((OWN, 5)),
            dma((2, 3)),
            dma((2, 2)),
            dma((2, 2)),
            dma((2,)),
            dma((2,)),
            dma((DEEP, 2)),
            dma((DEEP, 2)),
            dma((DEEP, 2)),
            dma((DEEP, 2)),
            dma((n - 1,)),
            dma((n - 1,)),
            plain,
            plain((2,)),
            plain((2,)),
        ],
        compiler_params=pltpu.CompilerParams(collective_id=0, has_side_effects=True, vmem_limit_bytes=67043328),
        cost_estimate=pl.CostEstimate(
            flops=30 * tokens * d * ff, bytes_accessed=200_000_000, transcendentals=2 * layers * tokens * ff
        ),
    )(x, dy, wg, wu, wd)
    return out[4:7], out[7].reshape(())


def adamw(w, m, v, g):
    m = 0.9 * m + 0.1 * g
    v = 0.95 * v + 0.05 * g * g
    step = m * lax.rsqrt(v + 1e-8) + 0.1 * w
    return (w - 0.02 * step).astype(BF16), m, v


def solution(mesh):
    n = mesh.shape["dp"]

    def step(x, dy, *arrays):
        weights, m, v = (arrays[i : i + 3] for i in (0, 3, 6))
        gradients, factor = gradients_of(n, x[0], dy[0], *weights)
        new = [
            adamw(w.astype(F32), m, v, g.astype(F32) * factor) for w, m, v, g in zip(weights, m, v, gradients, strict=True)
        ]
        return tuple(one[which] for which in range(3) for one in new)

    states, cut = P(("rep", "dp"), None, None), P(None, "dp", None)
    return jax.shard_map(
        step,
        mesh=mesh,
        in_specs=(states, states) + (cut,) * 9,
        out_specs=(P("rep", "dp", None),) * 9,
        check_vma=False,
    )
```
